32 devices in a mesh: pop: 8 (over z, x), mp: 4 (over y, core).
Axes of the slice: x: 2, y: 2, z: 4, core: 2. Of those that a mesh axis runs over, the one named last changes fastest.
Arguments:
- tokens: bfloat16 [256, 3584], replicated, may hold values from -60 to 60
- target: bfloat16 [256, 3584], P(None, 'mp'), may hold values from -6 to 6
- w_query: bfloat16 [3584, 3584], P('pop', 'mp'), may hold values from -0.09375 to 0.09375
- w_key: bfloat16 [3584, 512], P(None, 'mp'), may hold values from -0.09375 to 0.09375
- w_value: bfloat16 [3584, 512], P(None, 'mp'), may hold values from -0.09375 to 0.09375
- w_out: bfloat16 [3584, 3584], P('mp', 'pop'), may hold values from -0.09375 to 0.09375
- query_left_factors: bfloat16 [8, 3584, 4], P('pop'), may hold values from -0.09375 to 0.09375
- query_right_factors: bfloat16 [8, 4, 3584], P('pop', None, 'mp'), may hold values from -6 to 6
- o_left: bfloat16 [8, 3584, 4], P('pop', 'mp'), may hold values from -0.09375 to 0.09375
- o_right: bfloat16 [8, 4, 3584], P('pop'), may hold values from -6 to 6
- member_ids: int32 [8], P('pop'), may hold values from 0 to 7, each once
Outputs:
- grad_query: float32 [3584, 3584], P('pop', 'mp')
- grad_out: float32 [3584, 3584], P('mp', 'pop')
- fitness: float32 [8], P('pop')
The draws below stay inside these ranges and needn't reach their ends.
Inputs may be any that keep to these rules, and one draw needn't show every extreme that they name: `member_ids`: every number from 0 to 7 appears once.
All inputs are finite; a program needn't handle non-finite values.
Results may differ from the reference program's by a relative error of at most 0.005.
Values may be sent and summed in bfloat16 or wider, within the bound.
A program may use at most 64 MiB of HBM per device.

```python
import math
import jax
import jax.numpy as jnp
from jax import lax

D = 3584
HEADS = 28
KV_HEADS = 4
HEAD_DIM = 128
RANK = 4
TOK = 256
F = 3584
KVF = 512
M = 8
N_MP = 4


def draw_tokens(key, part):
    first = jax.random.fold_in(key, 0)
    normal = jax.random.normal(first, (TOK, D), jnp.float32)
    return jnp.clip(normal, -5.0, 5.0).astype(jnp.bfloat16)


def level_of(stream_key, dims, cuts, low, largest):
    def one(axis_at, parts):
        draws = jax.random.uniform(jax.random.fold_in(jax.random.fold_in(stream_key, 6), axis_at), (parts,), jnp.float32, low / len(cuts), largest / len(cuts))
        return jnp.repeat(jnp.exp(draws), dims[axis_at] // parts).reshape((-1,) + (1,) * (len(dims) - axis_at - 1))

    gain = one(*cuts[0])
    for cut in cuts[1:]:
        gain = gain * one(*cut)
    return gain


def normal_values(stream_key, shape, scale, bound, shards=(), held_as=jnp.bfloat16):
    result = scale * jax.random.normal(stream_key, shape, jnp.float32)
    if shards:
        result = result * level_of(stream_key, shape, shards, -0.22, 0.18)
    return jnp.clip(result, -bound, bound).astype(held_as)


def setup_inputs(seed: int = 0) -> dict:
    key_list = jax.random.split(jax.random.key(seed), 12)
    return {
        "tokens": draw_tokens(jax.random.fold_in(key_list[11], 71), 0),
        "target": normal_values(key_list[1], (TOK, D), 1.0, 6.0, ((1, 4),)),
        "w_query": normal_values(key_list[2], (D, F), D ** -0.5, 0.09375, ((0, 8), (1, 4))),
        "w_key": normal_values(key_list[3], (D, KVF), D ** -0.5, 0.09375, ((1, 4),)),
        "w_value": normal_values(key_list[4], (D, KVF), D ** -0.5, 0.09375, ((1, 4),)),
        "w_out": normal_values(key_list[5], (F, D), F ** -0.5, 0.09375, ((0, 4), (1, 8))),
        "query_left_factors": normal_values(key_list[6], (M, D, RANK), D ** -0.5, 0.09375, ((0, 8),)),
        "query_right_factors": normal_values(key_list[7], (M, RANK, F), 1.0, 6.0, ((0, 8), (2, 4))),
        "o_left": normal_values(key_list[8], (M, F, RANK), F ** -0.5, 0.09375, ((0, 8), (1, 4))),
        "o_right": normal_values(key_list[9], (M, RANK, D), 1.0, 6.0, ((0, 8),)),
        "member_ids": jax.random.permutation(key_list[10], M).astype(jnp.int32),
    }


noise_scale = 0.5
rope_base = 1000000.0
spread_floor = 0.001

def tables(count, head_size):
    position = jnp.arange(count, dtype=jnp.float32)
    index = jnp.arange(head_size // 2, dtype=jnp.float32)
    freq = jnp.exp(-math.log(rope_base) * 2.0 * index / head_size)
    angle = position[:, None] * freq[None, :]
    return (jnp.cos(angle)[:, None, :], jnp.sin(angle)[:, None, :])

def rotate(field, cosine_table, sine):
    half = field.shape[-1] // 2
    first = field[..., :half]
    second = field[..., half:]
    return jnp.concatenate([first * cosine_table - second * sine, second * cosine_table + first * sine], axis=-1)

def reference(tokens, target, w_query, w_key, w_value, w_out, query_left_factors, query_right_factors, o_left, o_right, member_ids):
    tok = tokens.shape[0]
    width = tokens.shape[1]
    hidden = w_query.shape[1]
    members = query_left_factors.shape[0]
    group = HEADS // KV_HEADS
    block = hidden // N_MP
    scale = HEAD_DIM ** (-0.5)
    cosine_table, sine = tables(tok, HEAD_DIM)
    base = jnp.dot(tokens, w_query, preferred_element_type=jnp.float32)
    keys = rotate(jnp.dot(tokens, w_key, preferred_element_type=jnp.float32).reshape(tok, KV_HEADS, HEAD_DIM), cosine_table, sine).astype(jnp.bfloat16)
    values = jnp.dot(tokens, w_value, preferred_element_type=jnp.float32).astype(jnp.bfloat16).reshape(tok, KV_HEADS, HEAD_DIM)
    signs = (1 - 2 * (member_ids % 2)).astype(jnp.float32)
    causal = jnp.arange(tok)[:, None] >= jnp.arange(tok)[None, :]
    target_f = target.astype(jnp.float32)

    def score(index):
        sign = signs[index]
        lowrank_product = jnp.dot(tokens, query_left_factors[index], preferred_element_type=jnp.float32).astype(jnp.bfloat16)
        query = base + noise_scale * sign * jnp.dot(lowrank_product, query_right_factors[index], preferred_element_type=jnp.float32)
        query = rotate(query.reshape(tok, HEADS, HEAD_DIM), cosine_table, sine).astype(jnp.bfloat16)
        query = query.reshape(tok, KV_HEADS, group, HEAD_DIM)
        scores = jnp.einsum('tkgd,skd->kgts', query.astype(jnp.float32), keys.astype(jnp.float32)) * scale
        scores = jnp.where(causal, scores, -1e+30)
        probs = jax.nn.softmax(scores, axis=-1).astype(jnp.bfloat16)
        mixed = jnp.einsum('kgts,skd->tkgd', probs.astype(jnp.float32), values.astype(jnp.float32)).astype(jnp.bfloat16).reshape(tok, hidden)
        total = jnp.zeros((tok, width), jnp.float32)
        for part in range(N_MP):
            rows = mixed[:, part * block:(part + 1) * block]
            low_out = jnp.dot(rows, o_left[index, part * block:(part + 1) * block], preferred_element_type=jnp.float32)
            term = jnp.dot(rows, w_out[part * block:(part + 1) * block], preferred_element_type=jnp.float32)
            term = term + noise_scale * sign * jnp.dot(low_out, o_right[index].astype(jnp.float32), precision=lax.Precision.HIGHEST)
            rounded = lax.optimization_barrier(term.astype(jnp.bfloat16))
            total = total + rounded.astype(jnp.float32)
        diff = total - target_f
        return -(jnp.sum(diff * diff) / (tok * width))
    fitness = lax.map(score, jnp.arange(members))
    mean = jnp.sum(fitness) / members
    spread = jnp.sum((fitness - mean) * (fitness - mean)) / members
    weight = signs * (fitness - mean) / jnp.sqrt(spread + spread_floor)
    left_q = jnp.transpose(query_left_factors.astype(jnp.float32) * weight[:, None, None], (1, 0, 2)).reshape(width, members * RANK)
    right_q = query_right_factors.astype(jnp.float32).reshape(members * RANK, hidden)
    grad_query = jnp.dot(left_q, right_q, precision=lax.Precision.HIGHEST) / noise_scale
    output_left_factor = jnp.transpose(o_left.astype(jnp.float32) * weight[:, None, None], (1, 0, 2)).reshape(hidden, members * RANK)
    right_o = o_right.astype(jnp.float32).reshape(members * RANK, width)
    grad_out = jnp.dot(output_left_factor, right_o, precision=lax.Precision.HIGHEST) / noise_scale
    return (grad_query, grad_out, fitness)
```

```python
import functools
import math

import jax
import jax.numpy as jnp
import numpy as np
from jax import lax
from jax.experimental import pallas as pl
from jax.experimental.pallas import tpu as pltpu
from jax.sharding import PartitionSpec as P

HEAD_DIM = 128
RANK = 4
PACK = 16
LINK = jnp.float32

noise_scale = 0.5
rope_base = 1000000.0
spread_floor = 0.001
MESH = pl.DeviceIdType.MESH
f32 = jnp.float32
bf16 = jnp.bfloat16


def rope_tables(count, head_size):
    index = np.arange(head_size // 2, dtype=np.float64)
    freq = np.exp(-math.log(rope_base) * 2.0 * index / head_size)
    angle = np.arange(count, dtype=np.float64)[:, None] * freq[None, :]
    cosine, sine = np.cos(angle), np.sin(angle)
    return (
        np.concatenate([cosine, cosine], 1).astype(np.float32),
        np.concatenate([-sine, sine], 1).astype(np.float32),
    )


def dot(a, b, dims=((1,), (0,))):
    return lax.dot_general(a, b, (dims, ((), ())), preferred_element_type=f32)


def split3(x):
    hi = x.astype(bf16)
    rest = x - hi.astype(f32)
    mid = rest.astype(bf16)
    low = (rest - mid.astype(f32)).astype(bf16)
    return hi, mid, low


def shift_half(pack):
    rows = pack.shape[0]
    row = lax.broadcasted_iota(jnp.int32, (rows, rows), 0)
    col = lax.broadcasted_iota(jnp.int32, (rows, rows), 1)
    perm = ((col == row + PACK // 2) & (row % PACK < PACK // 2)).astype(bf16)
    return dot(perm, pack).astype(bf16)


def forward_kernel(
    n_pop, n_mp, width,
    tok_ref, tokp_ref, wq_ref, wk_ref, wv_ref, wo_ref, qlt_ref, pkg_ref, tgt_ref, cos_ref, sin_ref,
    pack_out, stat_out,
    part, parts_in, lowq, lowq_in, packs, ring, terms, terms_in, target, errs, shifted,
    base_send, base_recv, lowq_send, lowq_recv, pack_send, pack_recv,
    ring_send, ring_recv, term_send, term_recv, tgt_send, tgt_recv, err_send, err_recv,
):
    me = lax.axis_index("pop")
    mc = lax.axis_index("mp")
    n_dev = n_pop * n_mp
    tok, feats = part.shape[0] * part.shape[1], part.shape[2]
    own_tok = tok // n_pop
    rows = n_pop * own_tok
    half = rows // 2
    per_mp = rows // n_mp
    heads = feats // HEAD_DIM
    cols = wo_ref.shape[1]

    barrier = pltpu.get_barrier_semaphore()

    def greet(i, carry):
        other = lax.rem(mc * n_pop + me + i, n_dev)
        pl.semaphore_signal(
            barrier, inc=1,
            device_id={"pop": lax.rem(other, n_pop), "mp": other // n_pop},
            device_id_type=MESH,
        )
        return carry

    lax.fori_loop(1, n_dev, greet, 0)

    part[...] = dot(tokp_ref[...], wq_ref[...]).reshape(part.shape).astype(part.dtype)
    low = dot(tok_ref[...], qlt_ref[...], ((1,), (1,))).astype(bf16)
    row = lax.broadcasted_iota(jnp.int32, (PACK, 128), 0)
    lane = lax.broadcasted_iota(jnp.int32, (PACK, 128), 1)
    spread_lanes = (lane == me * PACK + row).astype(bf16)
    lowq[...] = dot(low, spread_lanes).astype(bf16).reshape(lowq.shape)
    parts_in[me] = part[me]
    lowq_in[me] = lowq[me]
    packs[me] = pkg_ref[me]

    pl.semaphore_wait(barrier, n_dev - 1)

    def to_pop(i):
        other = lax.rem(me + i, n_pop)
        source = lax.rem(me + n_pop - i, n_pop)
        out = []
        for src, dst, send, recv in (
            (part, parts_in, base_send, base_recv),
            (lowq, lowq_in, lowq_send, lowq_recv),
            (pkg_ref, packs, pack_send, pack_recv),
        ):
            out.append(
                (
                    pltpu.make_async_remote_copy(
                        src_ref=src.at[other], dst_ref=dst.at[me], send_sem=send.at[i],
                        recv_sem=recv.at[i], device_id={"pop": other}, device_id_type=MESH,
                    )
                )
            )
        return out

    for i in range(1, n_pop):
        for copy in to_pop(i):
            copy.start()

    owner = me // (n_pop // n_mp)

    def target_copy(i):
        return pltpu.make_async_remote_copy(
            src_ref=tgt_ref, dst_ref=target, send_sem=tgt_send.at[i], recv_sem=tgt_recv,
            device_id={"mp": lax.rem(mc + i, n_mp)}, device_id_type=MESH,
        )

    @pl.when(mc == owner)
    def _():
        for i in range(1, n_mp):
            target_copy(i).start()
        target[...] = tgt_ref[...]

    cosine, sine = cos_ref[...], sin_ref[...]
    key = dot(tok_ref[...], wk_ref[...])
    key = (key * cosine + pltpu.roll(key, HEAD_DIM // 2, 1) * sine).astype(bf16)
    value = dot(tok_ref[...], wv_ref[...]).astype(bf16)

    for i in range(1, n_pop):
        for copy in to_pop(i):
            copy.wait_recv()

    pack = packs[...].reshape(n_pop * PACK, feats)
    shifted[...] = shift_half(pack[:, :cols]) if cols % 128 == 0 else shift_half(pack)[:, :cols]

    def pop_at(r):
        r = lax.rem(r + 2 * n_pop, n_pop)
        return jnp.where(r < n_pop // 2, 2 * r, 2 * (n_pop - 1 - r) + 1)

    my_r = jnp.where(lax.rem(me, 2) == 0, me // 2, n_pop - 1 - me // 2)
    right, left = pop_at(my_r + 1), pop_at(my_r - 1)

    total = parts_in[0].astype(f32)
    for i in range(1, n_pop):
        total = total + parts_in[i].astype(f32)
    low_rows = lowq_in[...].reshape(rows, 128)
    start = pl.multiple_of(me * own_tok, own_tok)
    cos_own = jnp.tile(cos_ref[pl.ds(start, own_tok), :], (n_pop, 1))
    sin_own = jnp.tile(sin_ref[pl.ds(start, own_tok), :], (n_pop, 1))
    token_of = start + lax.rem(lax.broadcasted_iota(jnp.int32, (rows, tok), 0), own_tok)
    causal = token_of >= lax.broadcasted_iota(jnp.int32, (rows, tok), 1)
    scale = HEAD_DIM ** (-0.5)
    for h in range(heads):
        lanes = slice(h * HEAD_DIM, (h + 1) * HEAD_DIM)
        q = jnp.tile(total[:, lanes], (n_pop, 1)) + dot(low_rows, pack[:, lanes])
        q = (q * cos_own + pltpu.roll(q, HEAD_DIM // 2, 1) * sin_own).astype(bf16)
        s = dot(q, key, ((1,), (1,))) * scale
        s = jnp.where(causal, s, -1e30)
        e = jnp.exp(s - jnp.max(s, axis=1, keepdims=True))
        prob = (e / jnp.sum(e, axis=1, keepdims=True)).astype(bf16)
        mixed = dot(prob, value).astype(bf16)
        for g in range(2):
            ring[me, g, :, lanes] = mixed[g * half:(g + 1) * half]

    depth = n_pop // 2

    def hop(direction, step, g):
        at = pop_at(my_r - step if direction == 0 else my_r + step)
        return pltpu.make_async_remote_copy(
            src_ref=ring.at[at, g], dst_ref=ring.at[at, g],
            send_sem=ring_send.at[direction, step, g], recv_sem=ring_recv.at[direction, step, g],
            device_id={"pop": right if direction == 0 else left}, device_id_type=MESH,
        )

    def hops(direction, step, g):
        return step < depth - 1 or (step == depth - 1 and g == direction)

    def term_copy(at, slot, block, i):
        return pltpu.make_async_remote_copy(
            src_ref=terms.at[at, block], dst_ref=terms_in.at[mc, at],
            send_sem=term_send.at[at, block], recv_sem=term_recv.at[mc, at],
            device_id={"mp": block}, device_id_type=MESH,
        )

    per_half = n_mp // 2

    def project(at, g):
        x = ring[at, g]
        low = dot(x, pack, ((1,), (1,)))
        r = lax.broadcasted_iota(jnp.int32, low.shape, 0) // own_tok + g * (n_pop // 2)
        c = lax.broadcasted_iota(jnp.int32, low.shape, 1)
        keep = (c // PACK == r) & (lax.rem(c, PACK) >= RANK) & (lax.rem(c, PACK) < 2 * RANK)
        low = jnp.where(keep, low, 0.0)
        y = dot(x, wo_ref[...])
        for piece in split3(low):
            y = y + dot(piece, shifted[...])
        y = y.astype(bf16)
        for j in range(per_half):
            block = g * per_half + j
            terms[at, block] = y[j * per_mp:(j + 1) * per_mp]

            @pl.when(mc != block)
            def _():
                term_copy(at, None, block, None).start()

            @pl.when(mc == block)
            def _():
                terms_in[block, at] = terms[at, block]

    for g in range(2):
        for direction in range(2):
            hop(direction, 0, g).start()
    for g in range(2):
        project(me, g)
    for step in range(depth):
        for g in range(2):
            for direction in range(2):
                if hops(direction, step, g):
                    hop(direction, step, g).wait_recv()
                    if hops(direction, step + 1, g):
                        hop(direction, step + 1, g).start()
        for g in range(2):
            for direction in range(2):
                if hops(direction, step, g):
                    project(pop_at(my_r - 1 - step if direction == 0 else my_r + 1 + step), g)

    @pl.when(mc != owner)
    def _():
        target_copy(1).wait_recv()

    for i in range(1, n_mp):
        source = lax.rem(mc + i, n_mp)
        for at in range(n_pop):
            pltpu.make_async_remote_copy(
                src_ref=terms.at[at, 0], dst_ref=terms_in.at[source, at],
                send_sem=term_send.at[at, 0], recv_sem=term_recv.at[source, at],
                device_id={"mp": source}, device_id_type=MESH,
            ).wait_recv()

    members = n_pop // n_mp
    lane_row = lax.broadcasted_iota(jnp.int32, (1, 128), 1)
    mine = jnp.zeros((1, 128), f32)
    for k in range(members):
        acc = jnp.zeros((own_tok, cols), f32)
        for at in range(n_pop):
            span = slice(k * own_tok, (k + 1) * own_tok)
            out = terms_in[0, at, span].astype(f32)
            for c in range(1, n_mp):
                out = out + terms_in[c, at, span].astype(f32)
            diff = out - target[at * own_tok:(at + 1) * own_tok].astype(f32)
            acc = acc + diff * diff
        value_k = jnp.sum(jnp.sum(acc, axis=1, keepdims=True), axis=0, keepdims=True)
        mine = mine + jnp.where(lane_row == mc * members + k, value_k, 0.0)

    my_id = mc * n_pop + me
    errs[my_id] = mine

    def err_copy(i):
        other = lax.rem(my_id + i, n_dev)
        return pltpu.make_async_remote_copy(
            src_ref=errs.at[my_id], dst_ref=errs.at[my_id],
            send_sem=err_send.at[i], recv_sem=err_recv.at[i],
            device_id={"pop": lax.rem(other, n_pop), "mp": other // n_pop}, device_id_type=MESH,
        )

    def err_start(i, carry):
        err_copy(i).start()
        return carry

    def err_wait(i, carry):
        err_copy(i).wait_recv()
        return carry

    lax.fori_loop(1, n_dev, err_start, 0)
    pack_out[...] = pack
    for i in range(1, n_pop):
        for copy in to_pop(i):
            copy.wait_send()
    for step in range(depth):
        for g in range(2):
            for direction in range(2):
                if hops(direction, step, g):
                    hop(direction, step, g).wait_send()
    for block in range(n_mp):
        @pl.when(mc != block)
        def _():
            for at in range(n_pop):
                term_copy(at, None, block, None).wait_send()

    @pl.when(mc == owner)
    def _():
        for i in range(1, n_mp):
            target_copy(i).wait_send()

    lax.fori_loop(1, n_dev, err_wait, 0)
    error = errs[0]
    for i in range(1, n_dev):
        error = error + errs[i]
    live = lane_row < n_pop
    fitness = -(error / (tok * width))
    mean = jnp.sum(jnp.where(live, fitness, 0.0), axis=1, keepdims=True) / n_pop
    dev = jnp.where(live, fitness - mean, 0.0)
    spread = jnp.sum(dev * dev, axis=1, keepdims=True) / n_pop
    weight = dev / jnp.sqrt(spread + spread_floor)
    stat_out[...] = jnp.concatenate(
        [fitness, weight, jnp.zeros((6, 128), f32)], axis=0
    )

    def err_drain(i, carry):
        err_copy(i).wait_send()
        return carry

    lax.fori_loop(1, n_dev, err_drain, 0)


def grad_kernel(pack_ref, stat_ref, gq_ref, go_ref):
    pack = pack_ref[...]
    rows = pack.shape[0]
    cols = go_ref.shape[1]
    shifted = shift_half(pack)
    row = lax.broadcasted_iota(jnp.int32, (rows, 128), 0)
    lane = lax.broadcasted_iota(jnp.int32, (rows, 128), 1)
    per_row = jnp.sum(jnp.where(lane == row // PACK, stat_ref[1:2, :], 0.0), axis=1, keepdims=True)
    per_row = per_row / (noise_scale * noise_scale)
    kind = lax.rem(lax.broadcasted_iota(jnp.int32, (rows, 1), 0), PACK)
    wq = jnp.where(kind < RANK, per_row, 0.0)
    wo = jnp.where((kind >= RANK) & (kind < 2 * RANK), per_row, 0.0)
    small = shifted[:, :cols]
    for which, weight in ((0, wq), (1, wo)):
        scaled = split3(small.astype(f32) * weight)
        if which == 0:
            gq_ref[...] = sum(dot(s, pack, ((0,), (0,))) for s in scaled)
        else:
            go_ref[...] = sum(dot(pack, s, ((0,), (0,))) for s in scaled)


def per_device_fast(
    n_pop, n_mp,
    tokens, target, w_query, w_key, w_value, w_out,
    query_left_factors, query_right_factors, o_left, o_right, member_ids,
):
    tok, width = tokens.shape
    rows_q, feats = w_query.shape
    cols = w_out.shape[1]
    own_tok = tok // n_pop
    rows = n_pop * own_tok
    me = lax.axis_index("pop")
    factor = (noise_scale * (1 - 2 * (member_ids % 2))).astype(bf16)[0]
    tok_cols = lax.dynamic_slice(tokens, (0, me * rows_q), (tok, rows_q))
    ratio = feats // cols
    tgt = lax.dynamic_slice(target, (0, lax.rem(me, ratio) * cols), (tok, cols))
    qr = query_right_factors[0] * factor
    olt = o_left[0].T
    qlt = query_left_factors[0].T
    orr = o_right[0] * factor
    every = lambda x: jnp.broadcast_to(x[None], (n_pop,) + x.shape)
    blocks = lambda x: jnp.pad(
        x.reshape(RANK, n_pop, cols).transpose(1, 0, 2), ((0, 0), (0, 0), (0, feats - cols))
    )
    pkg = jnp.concatenate([every(qr), every(olt), blocks(qlt), blocks(orr)], axis=1)
    qlt16 = jnp.pad(qlt, ((0, PACK - RANK), (0, 0)))
    cosine, sine = rope_tables(tok, HEAD_DIM)
    vmem = pl.BlockSpec(memory_space=pltpu.VMEM)
    dma = pltpu.SemaphoreType.DMA
    depth = n_pop // 2
    n_dev = n_pop * n_mp
    pack, stat = pl.pallas_call(
        functools.partial(forward_kernel, n_pop, n_mp, width),
        name="forward",
        out_shape=(
            jax.ShapeDtypeStruct((n_pop * PACK, feats), bf16),
            jax.ShapeDtypeStruct((8, 128), f32),
        ),
        in_specs=[vmem] * 11,
        out_specs=(vmem, vmem),
        scratch_shapes=[
            pltpu.VMEM((n_pop, own_tok, feats), LINK),
            pltpu.VMEM((n_pop, own_tok, feats), LINK),
            pltpu.VMEM((n_pop, own_tok, 128), bf16),
            pltpu.VMEM((n_pop, own_tok, 128), bf16),
            pltpu.VMEM((n_pop, PACK, feats), bf16),
            pltpu.VMEM((n_pop, 2, rows // 2, feats), bf16),
            pltpu.VMEM((n_pop, n_mp, rows // n_mp, cols), bf16),
            pltpu.VMEM((n_mp, n_pop, rows // n_mp, cols), bf16),
            pltpu.VMEM((tok, cols), bf16),
            pltpu.VMEM((n_dev, 1, 128), f32),
            pltpu.VMEM((n_pop * PACK, cols), bf16),
            dma((n_pop,)), dma((n_pop,)), dma((n_pop,)), dma((n_pop,)), dma((n_pop,)), dma((n_pop,)),
            dma((2, depth, 2)), dma((2, depth, 2)),
            dma((n_pop, n_mp)), dma((n_mp, n_pop)),
            dma((n_mp,)), dma,
            dma((n_dev,)), dma((n_dev,)),
        ],
        compiler_params=pltpu.CompilerParams(
            collective_id=0, has_side_effects=True, vmem_limit_bytes=48 * 1024 * 1024
        ),
    )(tokens, tok_cols, w_query, w_key, w_value, w_out, qlt16, pkg, tgt,
      jnp.asarray(cosine), jnp.asarray(sine))
    grad_query, grad_out = pl.pallas_call(
        grad_kernel,
        name="grads",
        out_shape=(
            jax.ShapeDtypeStruct((cols, feats), f32),
            jax.ShapeDtypeStruct((feats, cols), f32),
        ),
        in_specs=[vmem, vmem],
        out_specs=(vmem, vmem),
    )(pack, stat)
    fitness = lax.dynamic_slice(stat[0], (me,), (1,))
    return grad_query, grad_out, fitness


def tables(count, head_size):
    position = jnp.arange(count, dtype=jnp.float32)
    index = jnp.arange(head_size // 2, dtype=jnp.float32)
    freq = jnp.exp(-math.log(rope_base) * 2.0 * index / head_size)
    angle = position[:, None] * freq[None, :]
    return (jnp.cos(angle)[:, None, :], jnp.sin(angle)[:, None, :])


def rotate(field, cosine_table, sine):
    half = field.shape[-1] // 2
    first = field[..., :half]
    second = field[..., half:]
    return jnp.concatenate(
        [first * cosine_table - second * sine, second * cosine_table + first * sine], axis=-1
    )


def per_device(
    tokens,
    target,
    w_query,
    w_key,
    w_value,
    w_out,
    query_left_factors,
    query_right_factors,
    o_left,
    o_right,
    member_ids,
):
    tok = tokens.shape[0]
    local_feats = w_query.shape[1]
    local_kv = w_key.shape[1] // HEAD_DIM
    group = group_of(w_query, w_key)
    local_heads = local_kv * group
    slots = query_left_factors.shape[0]
    scale = HEAD_DIM ** (-0.5)
    cosine_table, sine = tables(tok, HEAD_DIM)
    base = jnp.dot(
        tokens,
        lax.all_gather(w_query, "pop", axis=0, tiled=True),
        preferred_element_type=jnp.float32,
    )
    keys = rotate(
        jnp.dot(tokens, w_key, preferred_element_type=jnp.float32).reshape(tok, local_kv, HEAD_DIM),
        cosine_table,
        sine,
    ).astype(jnp.bfloat16)
    values = (
        jnp.dot(tokens, w_value, preferred_element_type=jnp.float32)
        .astype(jnp.bfloat16)
        .reshape(tok, local_kv, HEAD_DIM)
    )
    signs = (1 - 2 * (member_ids % 2)).astype(jnp.float32)
    factor = noise_scale * signs[:, None, None]
    lowrank_product = jnp.einsum(
        "td,mdr->mtr", tokens, query_left_factors, preferred_element_type=jnp.float32
    ).astype(jnp.bfloat16)
    query = base[None] + factor * jnp.einsum(
        "olj,ojv->olv", lowrank_product, query_right_factors, preferred_element_type=jnp.float32
    )
    query = rotate(
        query.reshape(slots, tok, local_heads, HEAD_DIM), cosine_table[None], sine[None]
    ).astype(jnp.bfloat16)
    query = query.reshape(slots, tok, local_kv, group, HEAD_DIM)
    scores = jnp.einsum("mtkgd,skd->mkgts", query, keys, preferred_element_type=jnp.float32) * scale
    causal = jnp.arange(tok)[:, None] >= jnp.arange(tok)[None, :]
    scores = jnp.where(causal, scores, -1e30)
    probs = jax.nn.softmax(scores, axis=-1).astype(jnp.bfloat16)
    mixed = (
        jnp.einsum("mkgts,skd->mtkgd", probs, values, preferred_element_type=jnp.float32)
        .astype(jnp.bfloat16)
        .reshape(slots, tok, local_feats)
    )
    low_out = jnp.einsum("mtf,mfr->mtr", mixed, o_left, preferred_element_type=jnp.float32)
    right_full = o_right.astype(jnp.float32)
    part = jnp.einsum(
        "mtf,fe->mte",
        mixed,
        lax.all_gather(w_out, "pop", axis=1, tiled=True),
        preferred_element_type=jnp.float32,
    )
    term = part + factor * jnp.einsum(
        "mtr,mre->mte", low_out, right_full, precision=lax.Precision.HIGHEST
    )
    output = lax.psum_scatter(
        term.astype(jnp.bfloat16), "mp", scatter_dimension=2, tiled=True
    ).astype(jnp.float32)
    diff = output - target.astype(jnp.float32)[None]
    errors = lax.psum(jnp.sum(diff * diff, axis=(1, 2)), "mp")
    fitness = -(errors / (tok * tokens.shape[1]))
    count = slots * lax.axis_size("pop")
    mean = lax.psum(jnp.sum(fitness), "pop") / count
    spread = lax.psum(jnp.sum((fitness - mean) * (fitness - mean)), "pop") / count
    weight = signs * (fitness - mean) / jnp.sqrt(spread + spread_floor)
    every_weight = lax.all_gather(weight, "pop", axis=0, tiled=True)
    right_factors_gathered, left_all = (
        lax.all_gather(query_right_factors, "pop", axis=0, tiled=True),
        lax.all_gather(o_left, "pop", axis=0, tiled=True),
    )
    rows_q = lax.all_to_all(query_left_factors, "pop", split_axis=1, concat_axis=0, tiled=True)
    cols_o = lax.all_to_all(o_right, "pop", split_axis=2, concat_axis=0, tiled=True)
    whole_population = rows_q.shape[0]
    left_q = jnp.transpose(
        rows_q.astype(jnp.float32) * every_weight[:, None, None], (1, 0, 2)
    ).reshape(rows_q.shape[1], whole_population * RANK)
    right_q = right_factors_gathered.astype(jnp.float32).reshape(
        whole_population * RANK, local_feats
    )
    grad_query = jnp.dot(left_q, right_q, precision=lax.Precision.HIGHEST) / noise_scale
    output_left_factor = jnp.transpose(
        left_all.astype(jnp.float32) * every_weight[:, None, None], (1, 0, 2)
    ).reshape(local_feats, whole_population * RANK)
    right_o = cols_o.astype(jnp.float32).reshape(whole_population * RANK, cols_o.shape[2])
    grad_out = jnp.dot(output_left_factor, right_o, precision=lax.Precision.HIGHEST) / noise_scale
    return (grad_query, grad_out, fitness)


def group_of(w_query, w_key):
    return w_query.shape[1] // w_key.shape[1]


def pick(args, n_pop, n_mp):
    tok = args[0].shape[0]
    kernel = (
        args[6].shape[0] == n_pop
        and n_pop % (2 * n_mp) == 0
        and n_mp % 2 == 0
        and n_pop * PACK <= 128
        and tok % (n_pop * PACK) == 0
        and args[3].shape[1] == n_mp * HEAD_DIM
    )
    return functools.partial(per_device_fast, n_pop, n_mp) if kernel else per_device


def solution(mesh):
    placed = (
        P(),
        P(None, "mp"),
        P("pop", "mp"),
        P(None, "mp"),
        P(None, "mp"),
        P("mp", "pop"),
        P("pop", None, None),
        P("pop", None, "mp"),
        P("pop", "mp", None),
        P("pop", None, None),
        P("pop"),
    )
    n_pop, n_mp = mesh.shape["pop"], mesh.shape["mp"]

    def whole(*args):
        return jax.shard_map(
            pick(args, n_pop, n_mp),
            mesh=mesh,
            in_specs=placed,
            out_specs=(P("pop", "mp"), P("mp", "pop"), P("pop")),
            check_vma=False,
        )(*args)

    return whole
```

```python
import functools
import math

import jax
import jax.numpy as jnp
import numpy as np
from jax import lax
from jax.experimental import pallas as pl
from jax.experimental.pallas import tpu as pltpu
from jax.sharding import PartitionSpec as P

HEAD_DIM = 128
RANK = 4
PACK = 8
LINK = jnp.bfloat16

noise_scale = 0.5
rope_base = 1000000.0
spread_floor = 0.001
MESH = pl.DeviceIdType.MESH
f32 = jnp.float32
bf16 = jnp.bfloat16


def rope_tables(count, head_size):
    index = np.arange(head_size // 2, dtype=np.float64)
    freq = np.exp(-math.log(rope_base) * 2.0 * index / head_size)
    angle = np.arange(count, dtype=np.float64)[:, None] * freq[None, :]
    cosine, sine = np.cos(angle), np.sin(angle)
    return (
        np.concatenate([cosine, cosine], 1).astype(np.float32),
        np.concatenate([-sine, sine], 1).astype(np.float32),
    )


def dot(a, b, dims=((1,), (0,))):
    return lax.dot_general(a, b, (dims, ((), ())), preferred_element_type=f32)


def split3(x):
    hi = x.astype(bf16)
    rest = x - hi.astype(f32)
    mid = rest.astype(bf16)
    low = (rest - mid.astype(f32)).astype(bf16)
    return hi, mid, low


def forward_kernel(
    n_pop, n_mp, width,
    tok_hbm, wq_hbm, wk_hbm, wv_hbm, wo_hbm, tgt_hbm, ql_ref, qr_ref, ol_ref, or_ref, id_ref,
    cos_ref, sin_ref,
    pack_a_out, pack_b_out, stat_out,
    tok_ref, wq_ref, wk_ref, wv_ref, wo_ref, tgt_ref,
    part, parts_in, lowq, lowq_in, mine_a, packs_a, mine_b, packs_b, ring_a, ring_b,
    terms, terms_in, tgt_own, target, errs, load_sem,
    base_send, base_recv, lowq_send, lowq_recv, a_send, a_recv, b_send, b_recv,
    ring_send, ring_recv, term_send, term_recv, tgt_send, tgt_recv, err_send, err_recv,
):
    me = lax.axis_index("pop")
    mc = lax.axis_index("mp")
    n_dev = n_pop * n_mp
    tok, feats = part.shape[0] * part.shape[1], part.shape[2]
    own_tok = tok // n_pop
    rows = n_pop * own_tok
    per_mp = rows // n_mp
    heads = feats // HEAD_DIM
    cols = wo_ref.shape[0]
    members = n_pop // n_mp
    odd = lax.rem(me, 2) == 1

    loads = [
        pltpu.make_async_copy(src, dst, load_sem.at[i])
        for i, (src, dst) in enumerate((
            (tok_hbm, tok_ref), (wq_hbm, wq_ref), (wk_hbm, wk_ref), (wv_hbm, wv_ref),
            (tgt_hbm, tgt_ref), (wo_hbm, wo_ref),
        ))
    ]
    for load in loads:
        load.start()

    barrier = pltpu.get_barrier_semaphore()

    def greet(i, carry):
        other = lax.rem(mc * n_pop + me + i, n_dev)
        pl.semaphore_signal(
            barrier, inc=1,
            device_id={"pop": lax.rem(other, n_pop), "mp": other // n_pop},
            device_id_type=MESH,
        )
        return carry

    lax.fori_loop(1, n_dev, greet, 0)

    sign = 1 - 2 * lax.rem(id_ref[0], 2)
    factor = noise_scale * sign.astype(f32)
    mine_a[...] = jnp.concatenate(
        [qr_ref[...].astype(f32) * factor, ol_ref[...].astype(f32)], axis=0
    ).astype(bf16)
    both = jnp.concatenate(
        [ql_ref[...].astype(f32), or_ref[...].astype(f32) * factor], axis=0
    )
    for q in range(n_pop):
        mine_b[q] = both[:, q * cols:(q + 1) * cols].astype(bf16)

    loads[0].wait()
    loads[1].wait()
    window = tok_ref[:, pl.ds(pl.multiple_of(me // 2 * 2 * cols, 128), 2 * cols)]
    wq = wq_ref[...]
    first, second = window[:, :cols], window[:, cols:]
    part[...] = dot(jnp.where(odd, second, first), wq).reshape(part.shape).astype(part.dtype)
    low = dot(tok_ref[...], both.astype(bf16), ((1,), (1,))).astype(bf16)
    row = lax.broadcasted_iota(jnp.int32, (PACK, 128), 0)
    lane = lax.broadcasted_iota(jnp.int32, (PACK, 128), 1)
    spread_lanes = ((lane == me * PACK + row) & (row < RANK)).astype(bf16)
    lowq[...] = dot(low, spread_lanes).astype(bf16).reshape(lowq.shape)
    parts_in[me] = part[me]
    lowq_in[me] = lowq[me]
    packs_a[me] = mine_a[...]
    packs_b[me] = mine_b[me]

    pl.semaphore_wait(barrier, n_dev - 1)

    def to_pop(i, kind):
        other = lax.rem(me + i, n_pop)
        src, dst, send, recv = (
            (part.at[other], parts_in, base_send, base_recv),
            (lowq.at[other], lowq_in, lowq_send, lowq_recv),
            (mine_a, packs_a, a_send, a_recv),
            (mine_b.at[other], packs_b, b_send, b_recv),
        )[kind]
        return pltpu.make_async_remote_copy(
            src_ref=src, dst_ref=dst.at[me], send_sem=send.at[i],
            recv_sem=recv.at[i], device_id={"pop": other}, device_id_type=MESH,
        )

    for kind in (0, 1, 2, 3):
        for i in range(1, n_pop):
            to_pop(i, kind).start()

    owner = me // (n_pop // n_mp)

    def target_copy(i):
        return pltpu.make_async_remote_copy(
            src_ref=tgt_own, dst_ref=target, send_sem=tgt_send.at[i], recv_sem=tgt_recv,
            device_id={"mp": lax.rem(mc + i, n_mp)}, device_id_type=MESH,
        )

    loads[4].wait()

    @pl.when(mc == owner)
    def _():
        tgt_own[...] = jnp.where(odd, tgt_ref[:, cols:], tgt_ref[:, :cols])
        for i in range(1, n_mp):
            target_copy(i).start()
        target[...] = tgt_own[...]

    loads[2].wait()
    loads[3].wait()
    cosine, sine = cos_ref[...], sin_ref[...]
    key = dot(tok_ref[...], wk_ref[...])
    key = (key * cosine + pltpu.roll(key, HEAD_DIM // 2, 1) * sine).astype(bf16)
    value = dot(tok_ref[...], wv_ref[...]).astype(bf16)

    start = pl.multiple_of(me * own_tok, own_tok)
    cos_own = jnp.tile(cos_ref[pl.ds(start, own_tok), :], (n_pop, 1))
    sin_own = jnp.tile(sin_ref[pl.ds(start, own_tok), :], (n_pop, 1))
    token_of = start + lax.rem(lax.broadcasted_iota(jnp.int32, (rows, tok), 0), own_tok)
    causal = token_of >= lax.broadcasted_iota(jnp.int32, (rows, tok), 1)
    scale = HEAD_DIM ** (-0.5)

    for kind in (0, 1, 2):
        for i in range(1, n_pop):
            to_pop(i, kind).wait_recv()

    def pop_at(r):
        r = lax.rem(r + 2 * n_pop, n_pop)
        return jnp.where(r < n_pop // 2, 2 * r, 2 * (n_pop - 1 - r) + 1)

    my_r = jnp.where(odd, n_pop - 1 - me // 2, me // 2)
    right, left = pop_at(my_r + 1), pop_at(my_r - 1)

    depth = n_pop // 2
    rings = (ring_a, ring_b)

    def hop(direction, step, g):
        at = pop_at(my_r - step if direction == 0 else my_r + step)
        return pltpu.make_async_remote_copy(
            src_ref=rings[g].at[at], dst_ref=rings[g].at[at],
            send_sem=ring_send.at[direction, step, g], recv_sem=ring_recv.at[direction, step, g],
            device_id={"pop": right if direction == 0 else left}, device_id_type=MESH,
        )

    def hops(direction, step, g):
        return step < depth - 1 or (step == depth - 1 and g == direction)

    pack_a = jnp.concatenate([packs_a[i].astype(f32) for i in range(n_pop)], axis=0).astype(bf16)
    low_rows = lowq_in[...].reshape(rows, 128)[:, :n_pop * PACK]
    group = ring_a.shape[2] // HEAD_DIM
    for h in range(heads):
        lanes = slice(h * HEAD_DIM, (h + 1) * HEAD_DIM)
        total = parts_in[0, :, lanes].astype(f32)
        for i in range(1, n_pop):
            total = total + parts_in[i, :, lanes].astype(f32)
        q = jnp.tile(total, (n_pop, 1)) + dot(low_rows, pack_a[:, lanes])
        q = (q * cos_own + pltpu.roll(q, HEAD_DIM // 2, 1) * sin_own).astype(bf16)
        s = dot(q, key, ((1,), (1,))) * scale
        s = jnp.where(causal, s, -1e30)
        e = jnp.exp(s - jnp.max(s, axis=1, keepdims=True))
        prob = (e / jnp.sum(e, axis=1, keepdims=True)).astype(bf16)
        mixed = dot(prob, value).astype(bf16)
        g = 0 if h < group else 1
        at = h - g * group
        rings[g][me, :, at * HEAD_DIM:(at + 1) * HEAD_DIM] = mixed
        if h in (group - 1, heads - 1):
            for direction in range(2):
                hop(direction, 0, g).start()

    for i in range(1, n_pop):
        to_pop(i, 3).wait_recv()
    pack_b = jnp.concatenate([packs_b[i].astype(f32) for i in range(n_pop)], axis=0).astype(bf16)
    pack_a_out[...] = pack_a
    pack_b_out[...] = pack_b
    loads[5].wait()

    def term_copy(at, block):
        return pltpu.make_async_remote_copy(
            src_ref=terms.at[at, block], dst_ref=terms_in.at[mc, at],
            send_sem=term_send.at[at, block], recv_sem=term_recv.at[mc, at],
            device_id={"mp": block}, device_id_type=MESH,
        )

    low_shape = (rows, n_pop * PACK)
    member_of = lax.broadcasted_iota(jnp.int32, low_shape, 0) // own_tok
    place = lax.broadcasted_iota(jnp.int32, low_shape, 1)
    keep = (place // PACK == member_of) & (lax.rem(place, PACK) >= RANK)
    cut = group * HEAD_DIM

    def project(at):
        xa, xb = ring_a[at], ring_b[at]
        nt = ((1,), (1,))
        low = dot(xa, pack_a[:, :cut], nt) + dot(xb, pack_a[:, cut:], nt)
        low = jnp.where(keep, low, 0.0)
        y = dot(xa, wo_ref[:, :cut], nt) + dot(xb, wo_ref[:, cut:], nt)
        for piece in split3(low):
            y = y + dot(piece, pack_b)
        y = y.astype(bf16)
        for block in range(n_mp):
            terms[at, block] = y[block * per_mp:(block + 1) * per_mp]

            @pl.when(mc != block)
            def _():
                term_copy(at, block).start()

            @pl.when(mc == block)
            def _():
                terms_in[block, at] = terms[at, block]

    def squares(at, totals):
        for i in range(1, n_mp):
            source = lax.rem(mc + i, n_mp)
            pltpu.make_async_remote_copy(
                src_ref=terms.at[at, 0], dst_ref=terms_in.at[source, at],
                send_sem=term_send.at[at, 0], recv_sem=term_recv.at[source, at],
                device_id={"mp": source}, device_id_type=MESH,
            ).wait_recv()
        goal = target[pl.ds(pl.multiple_of(at * own_tok, own_tok), own_tok), :].astype(f32)
        result = []
        for k in range(members):
            span = slice(k * own_tok, (k + 1) * own_tok)
            out = terms_in[0, at, span].astype(f32)
            for c in range(1, n_mp):
                out = out + terms_in[c, at, span].astype(f32)
            diff = out - goal
            result.append(totals[k] + jnp.sum(diff * diff, axis=0, keepdims=True))
        return result

    project(me)

    @pl.when(mc != owner)
    def _():
        target_copy(1).wait_recv()

    totals = [jnp.zeros((1, cols), f32)] * members
    done = [me]
    for step in range(depth):
        for g in range(2):
            for direction in range(2):
                if hops(direction, step, g):
                    hop(direction, step, g).wait_recv()
                    if hops(direction, step + 1, g):
                        hop(direction, step + 1, g).start()
        landed = [pop_at(my_r - 1 - step)]
        if step < depth - 1:
            landed.append(pop_at(my_r + 1 + step))
        for at in landed:
            project(at)
        for at in done:
            totals = squares(at, totals)
        done = landed
    for at in done:
        totals = squares(at, totals)

    lane_row = lax.broadcasted_iota(jnp.int32, (1, 128), 1)
    mine = jnp.zeros((1, 128), f32)
    for k in range(members):
        value_k = jnp.sum(totals[k], axis=1, keepdims=True)
        mine = mine + jnp.where(lane_row == mc * members + k, value_k, 0.0)

    my_id = mc * n_pop + me
    errs[my_id] = mine

    def err_copy(i):
        other = lax.rem(my_id + i, n_dev)
        return pltpu.make_async_remote_copy(
            src_ref=errs.at[my_id], dst_ref=errs.at[my_id],
            send_sem=err_send.at[i], recv_sem=err_recv.at[i],
            device_id={"pop": lax.rem(other, n_pop), "mp": other // n_pop}, device_id_type=MESH,
        )

    def err_start(i, carry):
        err_copy(i).start()
        return carry

    def err_wait(i, carry):
        err_copy(i).wait_recv()
        return carry

    lax.fori_loop(1, n_dev, err_start, 0)
    for kind in range(4):
        for i in range(1, n_pop):
            to_pop(i, kind).wait_send()
    for step in range(depth):
        for g in range(2):
            for direction in range(2):
                if hops(direction, step, g):
                    hop(direction, step, g).wait_send()
    for block in range(n_mp):
        @pl.when(mc != block)
        def _():
            for at in range(n_pop):
                term_copy(at, block).wait_send()

    @pl.when(mc == owner)
    def _():
        for i in range(1, n_mp):
            target_copy(i).wait_send()

    lax.fori_loop(1, n_dev, err_wait, 0)
    error = errs[0]
    for i in range(1, n_dev):
        error = error + errs[i]
    live = lane_row < n_pop
    fitness = -(error / (tok * width))
    mean = jnp.sum(jnp.where(live, fitness, 0.0), axis=1, keepdims=True) / n_pop
    dev = jnp.where(live, fitness - mean, 0.0)
    spread = jnp.sum(dev * dev, axis=1, keepdims=True) / n_pop
    weight = dev / jnp.sqrt(spread + spread_floor)
    stat_out[...] = jnp.concatenate(
        [fitness, weight, jnp.zeros((6, 128), f32)], axis=0
    )

    def err_drain(i, carry):
        err_copy(i).wait_send()
        return carry

    lax.fori_loop(1, n_dev, err_drain, 0)


def grad_kernel(a_ref, b_ref, stat_ref, gq_ref, got_ref):
    pack_a = a_ref[...]
    pack_b = b_ref[...].astype(f32)
    rows = pack_a.shape[0]
    row = lax.broadcasted_iota(jnp.int32, (rows, 128), 0)
    lane = lax.broadcasted_iota(jnp.int32, (rows, 128), 1)
    per_row = jnp.sum(jnp.where(lane == row // PACK, stat_ref[1:2, :], 0.0), axis=1, keepdims=True)
    per_row = per_row / (noise_scale * noise_scale)
    kind = lax.rem(lax.broadcasted_iota(jnp.int32, (rows, 1), 0), PACK)
    for out, weight in (
        (gq_ref, jnp.where(kind < RANK, per_row, 0.0)),
        (got_ref, jnp.where(kind >= RANK, per_row, 0.0)),
    ):
        out[...] = sum(dot(s, pack_a, ((0,), (0,))) for s in split3(pack_b * weight))


def per_device_fast(
    n_pop, n_mp,
    tokens, target, w_query, w_key, w_value, w_out,
    query_left_factors, query_right_factors, o_left, o_right, member_ids,
):
    tok, width = tokens.shape
    feats = w_query.shape[1]
    cols = w_out.shape[1]
    own_tok = tok // n_pop
    rows = n_pop * own_tok
    me = lax.axis_index("pop")
    cosine, sine = rope_tables(tok, HEAD_DIM)
    vmem = pl.BlockSpec(memory_space=pltpu.VMEM)
    hbm = pl.BlockSpec(memory_space=pltpu.HBM)
    smem = pl.BlockSpec(memory_space=pltpu.SMEM)
    dma = pltpu.SemaphoreType.DMA
    depth = n_pop // 2
    n_dev = n_pop * n_mp
    cut = (feats // HEAD_DIM + 1) // 2 * HEAD_DIM
    like = lambda x: pltpu.VMEM(x.shape, x.dtype)
    wot = w_out.T
    pack_a, pack_b, stat = pl.pallas_call(
        functools.partial(forward_kernel, n_pop, n_mp, width),
        name="forward",
        out_shape=(
            jax.ShapeDtypeStruct((n_pop * PACK, feats), bf16),
            jax.ShapeDtypeStruct((n_pop * PACK, cols), bf16),
            jax.ShapeDtypeStruct((8, 128), f32),
        ),
        in_specs=[hbm] * 6 + [vmem] * 4 + [smem] + [vmem] * 2,
        out_specs=(vmem, vmem, vmem),
        scratch_shapes=[
            like(tokens), like(w_query), like(w_key), like(w_value), like(wot), like(target),
            pltpu.VMEM((n_pop, own_tok, feats), LINK),
            pltpu.VMEM((n_pop, own_tok, feats), LINK),
            pltpu.VMEM((n_pop, own_tok, 128), bf16),
            pltpu.VMEM((n_pop, own_tok, 128), bf16),
            pltpu.VMEM((PACK, feats), bf16),
            pltpu.VMEM((n_pop, PACK, feats), bf16),
            pltpu.VMEM((n_pop, PACK, cols), bf16),
            pltpu.VMEM((n_pop, PACK, cols), bf16),
            pltpu.VMEM((n_pop, rows, cut), bf16),
            pltpu.VMEM((n_pop, rows, feats - cut), bf16),
            pltpu.VMEM((n_pop, n_mp, rows // n_mp, cols), bf16),
            pltpu.VMEM((n_mp, n_pop, rows // n_mp, cols), bf16),
            pltpu.VMEM((tok, cols), bf16),
            pltpu.VMEM((tok, cols), bf16),
            pltpu.VMEM((n_dev, 1, 128), f32),
            dma((6,)),
            dma((n_pop,)), dma((n_pop,)), dma((n_pop,)), dma((n_pop,)),
            dma((n_pop,)), dma((n_pop,)), dma((n_pop,)), dma((n_pop,)),
            dma((2, depth, 2)), dma((2, depth, 2)),
            dma((n_pop, n_mp)), dma((n_mp, n_pop)),
            dma((n_mp,)), dma,
            dma((n_dev,)), dma((n_dev,)),
        ],
        compiler_params=pltpu.CompilerParams(
            collective_id=0, has_side_effects=True, vmem_limit_bytes=60 * 1024 * 1024
        ),
    )(tokens, w_query, w_key, w_value, wot, target,
      query_left_factors[0].T, query_right_factors[0], o_left[0].T, o_right[0], member_ids,
      jnp.asarray(cosine), jnp.asarray(sine))
    grad_query, grad_out_t = pl.pallas_call(
        grad_kernel,
        name="grads",
        out_shape=(
            jax.ShapeDtypeStruct((cols, feats), f32),
            jax.ShapeDtypeStruct((cols, feats), f32),
        ),
        in_specs=[vmem, vmem, vmem],
        out_specs=(vmem, vmem),
    )(pack_a, pack_b, stat)
    fitness = lax.dynamic_slice(stat[0], (me,), (1,))
    return grad_query, grad_out_t.T, fitness


def tables(count, head_size):
    position = jnp.arange(count, dtype=jnp.float32)
    index = jnp.arange(head_size // 2, dtype=jnp.float32)
    freq = jnp.exp(-math.log(rope_base) * 2.0 * index / head_size)
    angle = position[:, None] * freq[None, :]
    return (jnp.cos(angle)[:, None, :], jnp.sin(angle)[:, None, :])


def rotate(field, cosine_table, sine):
    half = field.shape[-1] // 2
    first = field[..., :half]
    second = field[..., half:]
    return jnp.concatenate(
        [first * cosine_table - second * sine, second * cosine_table + first * sine], axis=-1
    )


def per_device(
    tokens,
    target,
    w_query,
    w_key,
    w_value,
    w_out,
    query_left_factors,
    query_right_factors,
    o_left,
    o_right,
    member_ids,
):
    tok = tokens.shape[0]
    local_feats = w_query.shape[1]
    local_kv = w_key.shape[1] // HEAD_DIM
    group = group_of(w_query, w_key)
    local_heads = local_kv * group
    slots = query_left_factors.shape[0]
    scale = HEAD_DIM ** (-0.5)
    cosine_table, sine = tables(tok, HEAD_DIM)
    base = jnp.dot(
        tokens,
        lax.all_gather(w_query, "pop", axis=0, tiled=True),
        preferred_element_type=jnp.float32,
    )
    keys = rotate(
        jnp.dot(tokens, w_key, preferred_element_type=jnp.float32).reshape(tok, local_kv, HEAD_DIM),
        cosine_table,
        sine,
    ).astype(jnp.bfloat16)
    values = (
        jnp.dot(tokens, w_value, preferred_element_type=jnp.float32)
        .astype(jnp.bfloat16)
        .reshape(tok, local_kv, HEAD_DIM)
    )
    signs = (1 - 2 * (member_ids % 2)).astype(jnp.float32)
    factor = noise_scale * signs[:, None, None]
    lowrank_product = jnp.einsum(
        "td,mdr->mtr", tokens, query_left_factors, preferred_element_type=jnp.float32
    ).astype(jnp.bfloat16)
    query = base[None] + factor * jnp.einsum(
        "olj,ojv->olv", lowrank_product, query_right_factors, preferred_element_type=jnp.float32
    )
    query = rotate(
        query.reshape(slots, tok, local_heads, HEAD_DIM), cosine_table[None], sine[None]
    ).astype(jnp.bfloat16)
    query = query.reshape(slots, tok, local_kv, group, HEAD_DIM)
    scores = jnp.einsum("mtkgd,skd->mkgts", query, keys, preferred_element_type=jnp.float32) * scale
    causal = jnp.arange(tok)[:, None] >= jnp.arange(tok)[None, :]
    scores = jnp.where(causal, scores, -1e30)
    probs = jax.nn.softmax(scores, axis=-1).astype(jnp.bfloat16)
    mixed = (
        jnp.einsum("mkgts,skd->mtkgd", probs, values, preferred_element_type=jnp.float32)
        .astype(jnp.bfloat16)
        .reshape(slots, tok, local_feats)
    )
    low_out = jnp.einsum("mtf,mfr->mtr", mixed, o_left, preferred_element_type=jnp.float32)
    right_full = o_right.astype(jnp.float32)
    part = jnp.einsum(
        "mtf,fe->mte",
        mixed,
        lax.all_gather(w_out, "pop", axis=1, tiled=True),
        preferred_element_type=jnp.float32,
    )
    term = part + factor * jnp.einsum(
        "mtr,mre->mte", low_out, right_full, precision=lax.Precision.HIGHEST
    )
    output = lax.psum_scatter(
        term.astype(jnp.bfloat16), "mp", scatter_dimension=2, tiled=True
    ).astype(jnp.float32)
    diff = output - target.astype(jnp.float32)[None]
    errors = lax.psum(jnp.sum(diff * diff, axis=(1, 2)), "mp")
    fitness = -(errors / (tok * tokens.shape[1]))
    count = slots * lax.axis_size("pop")
    mean = lax.psum(jnp.sum(fitness), "pop") / count
    spread = lax.psum(jnp.sum((fitness - mean) * (fitness - mean)), "pop") / count
    weight = signs * (fitness - mean) / jnp.sqrt(spread + spread_floor)
    every_weight = lax.all_gather(weight, "pop", axis=0, tiled=True)
    right_factors_gathered, left_all = (
        lax.all_gather(query_right_factors, "pop", axis=0, tiled=True),
        lax.all_gather(o_left, "pop", axis=0, tiled=True),
    )
    rows_q = lax.all_to_all(query_left_factors, "pop", split_axis=1, concat_axis=0, tiled=True)
    cols_o = lax.all_to_all(o_right, "pop", split_axis=2, concat_axis=0, tiled=True)
    whole_population = rows_q.shape[0]
    left_q = jnp.transpose(
        rows_q.astype(jnp.float32) * every_weight[:, None, None], (1, 0, 2)
    ).reshape(rows_q.shape[1], whole_population * RANK)
    right_q = right_factors_gathered.astype(jnp.float32).reshape(
        whole_population * RANK, local_feats
    )
    grad_query = jnp.dot(left_q, right_q, precision=lax.Precision.HIGHEST) / noise_scale
    output_left_factor = jnp.transpose(
        left_all.astype(jnp.float32) * every_weight[:, None, None], (1, 0, 2)
    ).reshape(local_feats, whole_population * RANK)
    right_o = cols_o.astype(jnp.float32).reshape(whole_population * RANK, cols_o.shape[2])
    grad_out = jnp.dot(output_left_factor, right_o, precision=lax.Precision.HIGHEST) / noise_scale
    return (grad_query, grad_out, fitness)


def group_of(w_query, w_key):
    return w_query.shape[1] // w_key.shape[1]


def pick(args, n_pop, n_mp):
    tok = args[0].shape[0]
    kernel = (
        args[6].shape[0] == n_pop
        and n_pop % n_mp == 0
        and n_pop % 2 == 0
        and n_pop * PACK <= 128
        and tok % (n_pop * 16) == 0
        and args[2].shape[1] // n_mp == 2 * args[5].shape[1] // n_pop
        and args[2].shape[0] == args[5].shape[1]
        and args[3].shape[1] == n_mp * HEAD_DIM
    )
    return functools.partial(per_device_fast, n_pop, n_mp) if kernel else per_device


def solution(mesh):
    placed = (
        P(),
        P(None, "mp"),
        P("pop", "mp"),
        P(None, "mp"),
        P(None, "mp"),
        P("mp", "pop"),
        P("pop", None, None),
        P("pop", None, "mp"),
        P("pop", "mp", None),
        P("pop", None, None),
        P("pop"),
    )
    n_pop, n_mp = mesh.shape["pop"], mesh.shape["mp"]

    def whole(*args):
        return jax.shard_map(
            pick(args, n_pop, n_mp),
            mesh=mesh,
            in_specs=placed,
            out_specs=(P("pop", "mp"), P("mp", "pop"), P("pop")),
            check_vma=False,
        )(*args)

    return whole
```

```python
import functools
import math

import jax
import jax.numpy as jnp
import numpy as np
from jax import lax
from jax.experimental import pallas as pl
from jax.experimental.pallas import tpu as pltpu
from jax.sharding import PartitionSpec as P

HEAD_DIM = 128
RANK = 4
PACK = 8
LINK = jnp.bfloat16

noise_scale = 0.5
rope_base = 1000000.0
spread_floor = 0.001
MESH = pl.DeviceIdType.MESH
f32 = jnp.float32
bf16 = jnp.bfloat16


def rope_tables(count, head_size):
    index = np.arange(head_size // 2, dtype=np.float64)
    freq = np.exp(-math.log(rope_base) * 2.0 * index / head_size)
    angle = np.arange(count, dtype=np.float64)[:, None] * freq[None, :]
    cosine, sine = np.cos(angle), np.sin(angle)
    return (
        np.concatenate([cosine, cosine], 1).astype(np.float32),
        np.concatenate([-sine, sine], 1).astype(np.float32),
    )


def dot(a, b, dims=((1,), (0,))):
    return lax.dot_general(a, b, (dims, ((), ())), preferred_element_type=f32)


def split3(x):
    hi = x.astype(bf16)
    rest = x - hi.astype(f32)
    mid = rest.astype(bf16)
    low = (rest - mid.astype(f32)).astype(bf16)
    return hi, mid, low


def forward_kernel(
    n_pop, n_mp, width,
    tok_hbm, wq_hbm, wk_hbm, wv_hbm, wo_hbm, tgt_hbm, ql_ref, qr_ref, ol_ref, or_ref, id_ref,
    cos_ref, sin_ref,
    pack_a_out, pack_b_out, stat_out,
    tok_ref, wq_ref, wk_ref, wv_ref, wo_ref, tgt_ref,
    part_a, part_b, parts_a, parts_b, mine_l, packs_l, mine_q, packs_q, mine_o, packs_o,
    mine_b, packs_b, ring_a, ring_b,
    terms, terms_in, tgt_own, target, errs, load_sem,
    pop_send, pop_recv,
    ring_send, ring_recv, term_send, term_recv, tgt_send, tgt_recv, err_send, err_recv,
):
    me = lax.axis_index("pop")
    mc = lax.axis_index("mp")
    n_dev = n_pop * n_mp
    tok, feats = tok_ref.shape[0], wq_ref.shape[1]
    cut = ring_a.shape[2]
    own_tok = tok // n_pop
    rows = n_pop * own_tok
    per_mp = rows // n_mp
    heads = feats // HEAD_DIM
    cols = wo_ref.shape[0]
    members = n_pop // n_mp
    odd = lax.rem(me, 2) == 1

    loads = [
        pltpu.make_async_copy(src, dst, load_sem.at[i])
        for i, (src, dst) in enumerate((
            (tok_hbm, tok_ref), (wq_hbm, wq_ref), (wk_hbm, wk_ref), (wv_hbm, wv_ref),
            (tgt_hbm, tgt_ref), (wo_hbm, wo_ref),
        ))
    ]
    for load in loads:
        load.start()

    barrier = pltpu.get_barrier_semaphore()

    def greet(i, carry):
        other = lax.rem(mc * n_pop + me + i, n_dev)
        pl.semaphore_signal(
            barrier, inc=1,
            device_id={"pop": lax.rem(other, n_pop), "mp": other // n_pop},
            device_id_type=MESH,
        )
        return carry

    lax.fori_loop(1, n_dev, greet, 0)

    sign = 1 - 2 * lax.rem(id_ref[0], 2)
    factor = noise_scale * sign.astype(f32)
    loads[0].wait()
    loads[1].wait()
    window = tok_ref[:, pl.ds(pl.multiple_of(me // 2 * 2 * cols, 128), 2 * cols)]
    wq = wq_ref[...]
    first, second = window[:, :cols], window[:, cols:]
    base = dot(jnp.where(odd, second, first), wq)
    part_a[...] = base[:, :cut].reshape(part_a.shape).astype(LINK)
    part_b[...] = base[:, cut:].reshape(part_b.shape).astype(LINK)
    mine_q[...] = (qr_ref[...].astype(f32) * factor).astype(bf16)

    pl.semaphore_wait(barrier, n_dev - 1)

    def to_pop(i, kind):
        other = lax.rem(me + i, n_pop)
        src, dst = (
            (part_a.at[other], parts_a),
            (mine_q, packs_q),
            (mine_l.at[other], packs_l),
            (part_b.at[other], parts_b),
            (mine_o, packs_o),
            (mine_b.at[other], packs_b),
        )[kind]
        return pltpu.make_async_remote_copy(
            src_ref=src, dst_ref=dst.at[me], send_sem=pop_send.at[kind, i],
            recv_sem=pop_recv.at[kind, i], device_id={"pop": other}, device_id_type=MESH,
        )

    def to_all(kind):
        for i in range(1, n_pop):
            to_pop(i, kind).start()

    def from_all(kind):
        for i in range(1, n_pop):
            to_pop(i, kind).wait_recv()

    to_all(0)
    to_all(1)
    ql = ql_ref[...]
    low = dot(ql, tok_ref[...], ((1,), (1,))).astype(bf16).astype(f32)
    for q in range(n_pop):
        mine_l[q] = jnp.concatenate(
            [low[:, q * own_tok:(q + 1) * own_tok], jnp.zeros((RANK, 128 - own_tok), f32)], axis=1
        ).astype(bf16)
    to_all(2)
    to_all(3)
    mine_o[...] = ol_ref[...]
    both = jnp.concatenate([ql.astype(f32), or_ref[...].astype(f32) * factor], axis=0)
    for q in range(n_pop):
        mine_b[q] = both[:, q * cols:(q + 1) * cols].astype(bf16)
    to_all(4)
    to_all(5)
    for mine, packs in ((part_a, parts_a), (part_b, parts_b), (mine_l, packs_l), (mine_b, packs_b)):
        packs[me] = mine[me]
    packs_q[me] = mine_q[...]
    packs_o[me] = mine_o[...]

    owner = me // (n_pop // n_mp)

    def target_copy(i):
        return pltpu.make_async_remote_copy(
            src_ref=tgt_own, dst_ref=target, send_sem=tgt_send.at[i], recv_sem=tgt_recv,
            device_id={"mp": lax.rem(mc + i, n_mp)}, device_id_type=MESH,
        )

    loads[4].wait()

    @pl.when(mc == owner)
    def _():
        tgt_own[...] = jnp.where(odd, tgt_ref[:, cols:], tgt_ref[:, :cols])
        for i in range(1, n_mp):
            target_copy(i).start()
        target[...] = tgt_own[...]

    loads[2].wait()
    loads[3].wait()
    cosine, sine = cos_ref[...], sin_ref[...]
    key = dot(tok_ref[...], wk_ref[...])
    key = (key * cosine + pltpu.roll(key, HEAD_DIM // 2, 1) * sine).astype(bf16)
    value = dot(tok_ref[...], wv_ref[...]).astype(bf16)

    start = pl.multiple_of(me * own_tok, own_tok)
    cos_own = jnp.tile(cos_ref[pl.ds(start, own_tok), :], (n_pop, 1))
    sin_own = jnp.tile(sin_ref[pl.ds(start, own_tok), :], (n_pop, 1))
    token_of = start + lax.rem(lax.broadcasted_iota(jnp.int32, (rows, tok), 0), own_tok)
    causal = token_of >= lax.broadcasted_iota(jnp.int32, (rows, tok), 1)
    scale = HEAD_DIM ** (-0.5)

    for kind in range(3):
        from_all(kind)

    def pop_at(r):
        r = lax.rem(r + 2 * n_pop, n_pop)
        return jnp.where(r < n_pop // 2, 2 * r, 2 * (n_pop - 1 - r) + 1)

    my_r = jnp.where(odd, n_pop - 1 - me // 2, me // 2)
    right, left = pop_at(my_r + 1), pop_at(my_r - 1)

    depth = n_pop // 2
    rings = (ring_a, ring_b)

    def hop(direction, step, g):
        at = pop_at(my_r - step if direction == 0 else my_r + step)
        return pltpu.make_async_remote_copy(
            src_ref=rings[g].at[at], dst_ref=rings[g].at[at],
            send_sem=ring_send.at[direction, step, g], recv_sem=ring_recv.at[direction, step, g],
            device_id={"pop": right if direction == 0 else left}, device_id_type=MESH,
        )

    def hops(direction, step, g):
        return step < depth - 1 or (step == depth - 1 and g == direction)

    def stacked(parts, *more):
        return jnp.concatenate(
            [p[i].astype(f32) for i in range(n_pop) for p in (parts,) + more], axis=0
        ).astype(bf16)

    pack_q = stacked(packs_q)
    ranks = n_pop * RANK
    eye = (
        lax.broadcasted_iota(jnp.int32, (ranks, ranks), 0)
        == lax.broadcasted_iota(jnp.int32, (ranks, ranks), 1)
    ).astype(bf16)
    low_rows = dot(stacked(packs_l), eye, ((0,), (0,)))[:own_tok]
    low_rows = jnp.tile(low_rows, (n_pop, 1))
    of_rank = lax.broadcasted_iota(jnp.int32, low_rows.shape, 1) // RANK
    of_row = lax.broadcasted_iota(jnp.int32, low_rows.shape, 0) // own_tok
    low_rows = jnp.where(of_rank == of_row, low_rows, 0.0).astype(bf16)
    group = ring_a.shape[2] // HEAD_DIM
    for h in range(heads):
        lanes = slice(h * HEAD_DIM, (h + 1) * HEAD_DIM)
        g = 0 if h < group else 1
        at = h - g * group
        here = slice(at * HEAD_DIM, (at + 1) * HEAD_DIM)
        if h == group:
            from_all(3)
        parts = (parts_a, parts_b)[g]
        total = parts[0, :, here].astype(f32)
        for i in range(1, n_pop):
            total = total + parts[i, :, here].astype(f32)
        q = jnp.tile(total, (n_pop, 1)) + dot(low_rows, pack_q[:, lanes])
        q = (q * cos_own + pltpu.roll(q, HEAD_DIM // 2, 1) * sin_own).astype(bf16)
        s = dot(q, key, ((1,), (1,))) * scale
        s = jnp.where(causal, s, -1e30)
        e = jnp.exp(s - jnp.max(s, axis=1, keepdims=True))
        prob = (e / jnp.sum(e, axis=1, keepdims=True)).astype(bf16)
        mixed = dot(prob, value).astype(bf16)
        rings[g][me, :, here] = mixed
        if h in (group - 1, heads - 1):
            for direction in range(2):
                hop(direction, 0, g).start()

    from_all(4)
    from_all(5)
    pack_a = stacked(packs_q, packs_o)
    pack_b = stacked(packs_b)
    pack_a_out[...] = pack_a
    pack_b_out[...] = pack_b
    loads[5].wait()

    def term_copy(at, block):
        return pltpu.make_async_remote_copy(
            src_ref=terms.at[at, block], dst_ref=terms_in.at[mc, at],
            send_sem=term_send.at[at, block], recv_sem=term_recv.at[mc, at],
            device_id={"mp": block}, device_id_type=MESH,
        )

    low_shape = (rows, n_pop * PACK)
    member_of = lax.broadcasted_iota(jnp.int32, low_shape, 0) // own_tok
    place = lax.broadcasted_iota(jnp.int32, low_shape, 1)
    keep = (place // PACK == member_of) & (lax.rem(place, PACK) >= RANK)

    def project(at):
        xa, xb = ring_a[at], ring_b[at]
        nt = ((1,), (1,))
        low = dot(xa, pack_a[:, :cut], nt) + dot(xb, pack_a[:, cut:], nt)
        low = jnp.where(keep, low, 0.0)
        y = dot(xa, wo_ref[:, :cut], nt) + dot(xb, wo_ref[:, cut:], nt)
        for piece in split3(low):
            y = y + dot(piece, pack_b)
        y = y.astype(bf16)
        for block in range(n_mp):
            terms[at, block] = y[block * per_mp:(block + 1) * per_mp]

            @pl.when(mc != block)
            def _():
                term_copy(at, block).start()

            @pl.when(mc == block)
            def _():
                terms_in[block, at] = terms[at, block]

    def squares(at, totals):
        for i in range(1, n_mp):
            source = lax.rem(mc + i, n_mp)
            pltpu.make_async_remote_copy(
                src_ref=terms.at[at, 0], dst_ref=terms_in.at[source, at],
                send_sem=term_send.at[at, 0], recv_sem=term_recv.at[source, at],
                device_id={"mp": source}, device_id_type=MESH,
            ).wait_recv()
        goal = target[pl.ds(pl.multiple_of(at * own_tok, own_tok), own_tok), :].astype(f32)
        result = []
        for k in range(members):
            span = slice(k * own_tok, (k + 1) * own_tok)
            out = terms_in[0, at, span].astype(f32)
            for c in range(1, n_mp):
                out = out + terms_in[c, at, span].astype(f32)
            diff = out - goal
            result.append(totals[k] + jnp.sum(diff * diff, axis=0, keepdims=True))
        return result

    project(me)

    @pl.when(mc != owner)
    def _():
        target_copy(1).wait_recv()

    totals = [jnp.zeros((1, cols), f32)] * members
    done = [me]
    for step in range(depth):
        for g in range(2):
            for direction in range(2):
                if hops(direction, step, g):
                    hop(direction, step, g).wait_recv()
                    if hops(direction, step + 1, g):
                        hop(direction, step + 1, g).start()
        landed = [pop_at(my_r - 1 - step)]
        if step < depth - 1:
            landed.append(pop_at(my_r + 1 + step))
        for at in landed:
            project(at)
        for at in done:
            totals = squares(at, totals)
        done = landed
    for at in done:
        totals = squares(at, totals)

    lane_row = lax.broadcasted_iota(jnp.int32, (1, 128), 1)
    mine = jnp.zeros((1, 128), f32)
    for k in range(members):
        value_k = jnp.sum(totals[k], axis=1, keepdims=True)
        mine = mine + jnp.where(lane_row == mc * members + k, value_k, 0.0)

    my_id = mc * n_pop + me
    errs[my_id] = mine

    def err_copy(i):
        other = lax.rem(my_id + i, n_dev)
        return pltpu.make_async_remote_copy(
            src_ref=errs.at[my_id], dst_ref=errs.at[my_id],
            send_sem=err_send.at[i], recv_sem=err_recv.at[i],
            device_id={"pop": lax.rem(other, n_pop), "mp": other // n_pop}, device_id_type=MESH,
        )

    def err_start(i, carry):
        err_copy(i).start()
        return carry

    def err_wait(i, carry):
        err_copy(i).wait_recv()
        return carry

    lax.fori_loop(1, n_dev, err_start, 0)
    for kind in range(6):
        for i in range(1, n_pop):
            to_pop(i, kind).wait_send()
    for step in range(depth):
        for g in range(2):
            for direction in range(2):
                if hops(direction, step, g):
                    hop(direction, step, g).wait_send()
    for block in range(n_mp):
        @pl.when(mc != block)
        def _():
            for at in range(n_pop):
                term_copy(at, block).wait_send()

    @pl.when(mc == owner)
    def _():
        for i in range(1, n_mp):
            target_copy(i).wait_send()

    lax.fori_loop(1, n_dev, err_wait, 0)
    error = errs[0]
    for i in range(1, n_dev):
        error = error + errs[i]
    live = lane_row < n_pop
    fitness = -(error / (tok * width))
    mean = jnp.sum(jnp.where(live, fitness, 0.0), axis=1, keepdims=True) / n_pop
    dev = jnp.where(live, fitness - mean, 0.0)
    spread = jnp.sum(dev * dev, axis=1, keepdims=True) / n_pop
    weight = dev / jnp.sqrt(spread + spread_floor)
    stat_out[...] = jnp.concatenate(
        [fitness, weight, jnp.zeros((6, 128), f32)], axis=0
    )

    def err_drain(i, carry):
        err_copy(i).wait_send()
        return carry

    lax.fori_loop(1, n_dev, err_drain, 0)


def grad_kernel(a_ref, b_ref, stat_ref, gq_hbm, got_hbm, fit_ref, gq_ref, got_ref, sem):
    pack_a = a_ref[...]
    pack_b = b_ref[...].astype(f32)
    rows, cols = pack_b.shape
    row = lax.broadcasted_iota(jnp.int32, (rows, 128), 0)
    lane = lax.broadcasted_iota(jnp.int32, (rows, 128), 1)
    per_row = jnp.sum(jnp.where(lane == row // PACK, stat_ref[1:2, :], 0.0), axis=1, keepdims=True)
    per_row = per_row / (noise_scale * noise_scale)
    kind = lax.rem(lax.broadcasted_iota(jnp.int32, (rows, 1), 0), PACK)
    edges = (0, (cols // 2 + 127) // 128 * 128, cols)
    copies = []
    for out, target, weight in (
        (gq_ref, gq_hbm, jnp.where(kind < RANK, per_row, 0.0)),
        (got_ref, got_hbm, jnp.where(kind >= RANK, per_row, 0.0)),
    ):
        pieces = jnp.concatenate(split3(pack_b * weight), axis=0)
        right = jnp.concatenate([pack_a] * 3, axis=0)
        for low, high in zip(edges[:-1], edges[1:]):
            out[low:high, :] = dot(pieces[:, low:high], right, ((0,), (0,)))
            copy = pltpu.make_async_copy(
                out.at[low:high], target.at[low:high], sem.at[len(copies)]
            )
            copy.start()
            copies.append(copy)
    me = lax.axis_index("pop")
    fit_ref[0] = jnp.sum(jnp.where(lane[:1] == me, stat_ref[0:1, :], 0.0))
    for copy in copies:
        copy.wait()


def per_device_fast(
    n_pop, n_mp,
    tokens, target, w_query, w_key, w_value, w_out,
    query_left_factors, query_right_factors, o_left, o_right, member_ids,
):
    tok, width = tokens.shape
    feats = w_query.shape[1]
    cols = w_out.shape[1]
    own_tok = tok // n_pop
    rows = n_pop * own_tok
    cosine, sine = rope_tables(tok, HEAD_DIM)
    vmem = pl.BlockSpec(memory_space=pltpu.VMEM)
    hbm = pl.BlockSpec(memory_space=pltpu.HBM)
    smem = pl.BlockSpec(memory_space=pltpu.SMEM)
    dma = pltpu.SemaphoreType.DMA
    depth = n_pop // 2
    n_dev = n_pop * n_mp
    cut = (feats // HEAD_DIM + 1) // 2 * HEAD_DIM
    like = lambda x: pltpu.VMEM(x.shape, x.dtype)
    wot = w_out.T
    pack_a, pack_b, stat = pl.pallas_call(
        functools.partial(forward_kernel, n_pop, n_mp, width),
        name="forward",
        out_shape=(
            jax.ShapeDtypeStruct((n_pop * PACK, feats), bf16),
            jax.ShapeDtypeStruct((n_pop * PACK, cols), bf16),
            jax.ShapeDtypeStruct((8, 128), f32),
        ),
        in_specs=[hbm] * 6 + [vmem] * 4 + [smem] + [vmem] * 2,
        out_specs=(vmem, vmem, vmem),
        scratch_shapes=[
            like(tokens), like(w_query), like(w_key), like(w_value), like(wot), like(target),
            pltpu.VMEM((n_pop, own_tok, cut), LINK),
            pltpu.VMEM((n_pop, own_tok, feats - cut), LINK),
            pltpu.VMEM((n_pop, own_tok, cut), LINK),
            pltpu.VMEM((n_pop, own_tok, feats - cut), LINK),
            pltpu.VMEM((n_pop, RANK, 128), bf16),
            pltpu.VMEM((n_pop, RANK, 128), bf16),
            pltpu.VMEM((RANK, feats), bf16),
            pltpu.VMEM((n_pop, RANK, feats), bf16),
            pltpu.VMEM((RANK, feats), bf16),
            pltpu.VMEM((n_pop, RANK, feats), bf16),
            pltpu.VMEM((n_pop, PACK, cols), bf16),
            pltpu.VMEM((n_pop, PACK, cols), bf16),
            pltpu.VMEM((n_pop, rows, cut), bf16),
            pltpu.VMEM((n_pop, rows, feats - cut), bf16),
            pltpu.VMEM((n_pop, n_mp, rows // n_mp, cols), bf16),
            pltpu.VMEM((n_mp, n_pop, rows // n_mp, cols), bf16),
            pltpu.VMEM((tok, cols), bf16),
            pltpu.VMEM((tok, cols), bf16),
            pltpu.VMEM((n_dev, 1, 128), f32),
            dma((6,)),
            dma((6, n_pop)), dma((6, n_pop)),
            dma((2, depth, 2)), dma((2, depth, 2)),
            dma((n_pop, n_mp)), dma((n_mp, n_pop)),
            dma((n_mp,)), dma,
            dma((n_dev,)), dma((n_dev,)),
        ],
        compiler_params=pltpu.CompilerParams(
            collective_id=0, has_side_effects=True, vmem_limit_bytes=60 * 1024 * 1024
        ),
    )(tokens, w_query, w_key, w_value, wot, target,
      query_left_factors[0].T, query_right_factors[0], o_left[0].T, o_right[0], member_ids,
      jnp.asarray(cosine), jnp.asarray(sine))
    grad = jax.ShapeDtypeStruct((cols, feats), f32)
    grad_query, grad_out_t, fitness = pl.pallas_call(
        grad_kernel,
        name="grads",
        out_shape=(grad, grad, jax.ShapeDtypeStruct((1,), f32)),
        in_specs=[vmem, vmem, vmem],
        out_specs=(hbm, hbm, smem),
        scratch_shapes=[like(grad), like(grad), dma((4,))],
    )(pack_a, pack_b, stat)
    return grad_query, grad_out_t.T, fitness


def tables(count, head_size):
    position = jnp.arange(count, dtype=jnp.float32)
    index = jnp.arange(head_size // 2, dtype=jnp.float32)
    freq = jnp.exp(-math.log(rope_base) * 2.0 * index / head_size)
    angle = position[:, None] * freq[None, :]
    return (jnp.cos(angle)[:, None, :], jnp.sin(angle)[:, None, :])


def rotate(field, cosine_table, sine):
    half = field.shape[-1] // 2
    first = field[..., :half]
    second = field[..., half:]
    return jnp.concatenate(
        [first * cosine_table - second * sine, second * cosine_table + first * sine], axis=-1
    )


def per_device(
    tokens,
    target,
    w_query,
    w_key,
    w_value,
    w_out,
    query_left_factors,
    query_right_factors,
    o_left,
    o_right,
    member_ids,
):
    tok = tokens.shape[0]
    local_feats = w_query.shape[1]
    local_kv = w_key.shape[1] // HEAD_DIM
    group = group_of(w_query, w_key)
    local_heads = local_kv * group
    slots = query_left_factors.shape[0]
    scale = HEAD_DIM ** (-0.5)
    cosine_table, sine = tables(tok, HEAD_DIM)
    base = jnp.dot(
        tokens,
        lax.all_gather(w_query, "pop", axis=0, tiled=True),
        preferred_element_type=jnp.float32,
    )
    keys = rotate(
        jnp.dot(tokens, w_key, preferred_element_type=jnp.float32).reshape(tok, local_kv, HEAD_DIM),
        cosine_table,
        sine,
    ).astype(jnp.bfloat16)
    values = (
        jnp.dot(tokens, w_value, preferred_element_type=jnp.float32)
        .astype(jnp.bfloat16)
        .reshape(tok, local_kv, HEAD_DIM)
    )
    signs = (1 - 2 * (member_ids % 2)).astype(jnp.float32)
    factor = noise_scale * signs[:, None, None]
    lowrank_product = jnp.einsum(
        "td,mdr->mtr", tokens, query_left_factors, preferred_element_type=jnp.float32
    ).astype(jnp.bfloat16)
    query = base[None] + factor * jnp.einsum(
        "olj,ojv->olv", lowrank_product, query_right_factors, preferred_element_type=jnp.float32
    )
    query = rotate(
        query.reshape(slots, tok, local_heads, HEAD_DIM), cosine_table[None], sine[None]
    ).astype(jnp.bfloat16)
    query = query.reshape(slots, tok, local_kv, group, HEAD_DIM)
    scores = jnp.einsum("mtkgd,skd->mkgts", query, keys, preferred_element_type=jnp.float32) * scale
    causal = jnp.arange(tok)[:, None] >= jnp.arange(tok)[None, :]
    scores = jnp.where(causal, scores, -1e30)
    probs = jax.nn.softmax(scores, axis=-1).astype(jnp.bfloat16)
    mixed = (
        jnp.einsum("mkgts,skd->mtkgd", probs, values, preferred_element_type=jnp.float32)
        .astype(jnp.bfloat16)
        .reshape(slots, tok, local_feats)
    )
    low_out = jnp.einsum("mtf,mfr->mtr", mixed, o_left, preferred_element_type=jnp.float32)
    right_full = o_right.astype(jnp.float32)
    part = jnp.einsum(
        "mtf,fe->mte",
        mixed,
        lax.all_gather(w_out, "pop", axis=1, tiled=True),
        preferred_element_type=jnp.float32,
    )
    term = part + factor * jnp.einsum(
        "mtr,mre->mte", low_out, right_full, precision=lax.Precision.HIGHEST
    )
    output = lax.psum_scatter(
        term.astype(jnp.bfloat16), "mp", scatter_dimension=2, tiled=True
    ).astype(jnp.float32)
    diff = output - target.astype(jnp.float32)[None]
    errors = lax.psum(jnp.sum(diff * diff, axis=(1, 2)), "mp")
    fitness = -(errors / (tok * tokens.shape[1]))
    count = slots * lax.axis_size("pop")
    mean = lax.psum(jnp.sum(fitness), "pop") / count
    spread = lax.psum(jnp.sum((fitness - mean) * (fitness - mean)), "pop") / count
    weight = signs * (fitness - mean) / jnp.sqrt(spread + spread_floor)
    every_weight = lax.all_gather(weight, "pop", axis=0, tiled=True)
    right_factors_gathered, left_all = (
        lax.all_gather(query_right_factors, "pop", axis=0, tiled=True),
        lax.all_gather(o_left, "pop", axis=0, tiled=True),
    )
    rows_q = lax.all_to_all(query_left_factors, "pop", split_axis=1, concat_axis=0, tiled=True)
    cols_o = lax.all_to_all(o_right, "pop", split_axis=2, concat_axis=0, tiled=True)
    whole_population = rows_q.shape[0]
    left_q = jnp.transpose(
        rows_q.astype(jnp.float32) * every_weight[:, None, None], (1, 0, 2)
    ).reshape(rows_q.shape[1], whole_population * RANK)
    right_q = right_factors_gathered.astype(jnp.float32).reshape(
        whole_population * RANK, local_feats
    )
    grad_query = jnp.dot(left_q, right_q, precision=lax.Precision.HIGHEST) / noise_scale
    output_left_factor = jnp.transpose(
        left_all.astype(jnp.float32) * every_weight[:, None, None], (1, 0, 2)
    ).reshape(local_feats, whole_population * RANK)
    right_o = cols_o.astype(jnp.float32).reshape(whole_population * RANK, cols_o.shape[2])
    grad_out = jnp.dot(output_left_factor, right_o, precision=lax.Precision.HIGHEST) / noise_scale
    return (grad_query, grad_out, fitness)


def group_of(w_query, w_key):
    return w_query.shape[1] // w_key.shape[1]


def pick(args, n_pop, n_mp):
    tok = args[0].shape[0]
    kernel = (
        args[6].shape[0] == n_pop
        and n_pop % n_mp == 0
        and n_pop % 2 == 0
        and n_pop * PACK <= 128
        and tok % (n_pop * 16) == 0
        and tok // n_pop < 128
        and args[2].shape[1] // n_mp == 2 * args[5].shape[1] // n_pop
        and args[2].shape[0] == args[5].shape[1]
        and args[3].shape[1] == n_mp * HEAD_DIM
    )
    return functools.partial(per_device_fast, n_pop, n_mp) if kernel else per_device


def solution(mesh):
    placed = (
        P(),
        P(None, "mp"),
        P("pop", "mp"),
        P(None, "mp"),
        P(None, "mp"),
        P("mp", "pop"),
        P("pop", None, None),
        P("pop", None, "mp"),
        P("pop", "mp", None),
        P("pop", None, None),
        P("pop"),
    )
    n_pop, n_mp = mesh.shape["pop"], mesh.shape["mp"]

    def whole(*args):
        return jax.shard_map(
            pick(args, n_pop, n_mp),
            mesh=mesh,
            in_specs=placed,
            out_specs=(P("pop", "mp"), P("mp", "pop"), P("pop")),
            check_vma=False,
        )(*args)

    return whole
```

```python
import functools
import math

import jax
import jax.numpy as jnp
import numpy as np
from jax import lax
from jax.experimental import pallas as pl
from jax.experimental.pallas import tpu as pltpu
from jax.sharding import PartitionSpec as P

HEAD_DIM = 128
RANK = 4
PACK = 8
LINK = jnp.bfloat16

noise_scale = 0.5
rope_base = 1000000.0
spread_floor = 0.001
MESH = pl.DeviceIdType.MESH
f32 = jnp.float32
bf16 = jnp.bfloat16


def rope_tables(count, head_size):
    index = np.arange(head_size // 2, dtype=np.float64)
    freq = np.exp(-math.log(rope_base) * 2.0 * index / head_size)
    angle = np.arange(count, dtype=np.float64)[:, None] * freq[None, :]
    cosine, sine = np.cos(angle), np.sin(angle)
    return (
        np.concatenate([cosine, cosine], 1).astype(np.float32),
        np.concatenate([-sine, sine], 1).astype(np.float32),
    )


def head_groups(feats):
    heads = feats // HEAD_DIM
    return [(h * HEAD_DIM, min(h + 2, heads) * HEAD_DIM) for h in range(0, heads, 2)]


def dot(a, b, dims=((1,), (0,))):
    return lax.dot_general(a, b, (dims, ((), ())), preferred_element_type=f32)


def split3(x):
    hi = x.astype(bf16)
    rest = x - hi.astype(f32)
    mid = rest.astype(bf16)
    low = (rest - mid.astype(f32)).astype(bf16)
    return hi, mid, low


def forward_kernel(
    n_pop, n_mp, width,
    tok_hbm, wq_hbm, wk_hbm, wv_hbm, wo_hbm, tgt_hbm, ql_ref, qr_ref, ol_ref, or_ref, id_ref,
    cos_ref, sin_ref,
    pack_a_out, pack_b_out, stat_out,
    *refs,
):
    groups = head_groups(wq_hbm.shape[1])
    many = len(groups)
    tok_ref, window_ref, wq_ref, wkv_ref, wo_ref, tgt_ref = refs[:6]
    refs = refs[6:]
    mine_base, base_in, rings = refs[:many], refs[many:2 * many], refs[2 * many:3 * many]
    (
        mine_l, packs_l, mine_q, packs_q, mine_o, packs_o, mine_b, packs_b,
        terms, terms_in, tgt_own, target, errs, load_sem, pop_send, pop_recv,
        ring_send, ring_recv, term_send, term_recv, tgt_send, tgt_recv, err_send, err_recv,
    ) = refs[3 * many:]
    me = lax.axis_index("pop")
    mc = lax.axis_index("mp")
    n_dev = n_pop * n_mp
    tok, feats = tok_ref.shape[0], wq_ref.shape[1]
    own_tok = tok // n_pop
    rows = n_pop * own_tok
    per_mp = rows // n_mp
    heads = feats // HEAD_DIM
    cols = wo_ref.shape[0]
    members = n_pop // n_mp
    odd = lax.rem(me, 2) == 1

    kv_dim = wk_hbm.shape[1]
    around = pl.ds(pl.multiple_of(me // 2 * 2 * cols, 128), 2 * cols)
    loads = [
        pltpu.make_async_copy(src, dst, load_sem.at[i])
        for i, (src, dst) in enumerate((
            (wq_hbm, wq_ref), (tok_hbm.at[:, around], window_ref), (tok_hbm, tok_ref),
            (wk_hbm, wkv_ref.at[:, :kv_dim]), (wv_hbm, wkv_ref.at[:, kv_dim:]),
            (tgt_hbm, tgt_ref), (wo_hbm, wo_ref),
        ))
    ]
    for load in loads:
        load.start()

    barrier = pltpu.get_barrier_semaphore()

    def greet(i, carry):
        other = lax.rem(mc * n_pop + me + i, n_dev)
        pl.semaphore_signal(
            barrier, inc=1,
            device_id={"pop": lax.rem(other, n_pop), "mp": other // n_pop},
            device_id_type=MESH,
        )
        return carry

    lax.fori_loop(1, n_dev, greet, 0)

    sign = 1 - 2 * lax.rem(id_ref[0], 2)
    factor = noise_scale * sign.astype(f32)
    loads[0].wait()
    loads[1].wait()
    window = window_ref[...]
    wq = wq_ref[...]
    first, second = window[:, :cols], window[:, cols:]
    base = dot(jnp.where(odd, second, first), wq)
    for mine, (low, high) in zip(mine_base, groups):
        mine[...] = base[:, low:high].reshape(mine.shape).astype(LINK)
    mine_q[...] = (qr_ref[...].astype(f32) * factor).astype(bf16)

    pl.semaphore_wait(barrier, n_dev - 1)

    def to_pop(i, kind):
        other = lax.rem(me + i, n_pop)
        src, dst = (
            (mine_q, packs_q),
            (mine_l.at[other], packs_l),
            (mine_o, packs_o),
            (mine_b.at[other], packs_b),
            *((mine.at[other], landing) for mine, landing in zip(mine_base, base_in)),
        )[kind]
        return pltpu.make_async_remote_copy(
            src_ref=src, dst_ref=dst.at[me], send_sem=pop_send.at[kind, i],
            recv_sem=pop_recv.at[kind, i], device_id={"pop": other}, device_id_type=MESH,
        )

    def to_all(kind):
        for i in range(1, n_pop):
            to_pop(i, kind).start()

    def from_all(kind):
        for i in range(1, n_pop):
            to_pop(i, kind).wait_recv()

    to_all(4)
    to_all(0)
    loads[2].wait()
    ql = ql_ref[...]
    low = dot(ql, tok_ref[...], ((1,), (1,))).astype(bf16).astype(f32)
    for q in range(n_pop):
        mine_l[q] = jnp.concatenate(
            [low[:, q * own_tok:(q + 1) * own_tok], jnp.zeros((RANK, 128 - own_tok), f32)], axis=1
        ).astype(bf16)
    to_all(1)
    for g in range(1, many):
        to_all(4 + g)
    mine_o[...] = ol_ref[...]
    both = jnp.concatenate([ql.astype(f32), or_ref[...].astype(f32) * factor], axis=0)
    for q in range(n_pop):
        mine_b[q] = both[:, q * cols:(q + 1) * cols].astype(bf16)
    to_all(2)
    to_all(3)
    for mine, packs in (*zip(mine_base, base_in), (mine_l, packs_l), (mine_b, packs_b)):
        packs[me] = mine[me]
    packs_q[me] = mine_q[...]
    packs_o[me] = mine_o[...]

    owner = me // (n_pop // n_mp)

    def target_copy(i):
        return pltpu.make_async_remote_copy(
            src_ref=tgt_own, dst_ref=target, send_sem=tgt_send.at[i], recv_sem=tgt_recv,
            device_id={"mp": lax.rem(mc + i, n_mp)}, device_id_type=MESH,
        )

    loads[5].wait()

    @pl.when(mc == owner)
    def _():
        tgt_own[...] = jnp.where(odd, tgt_ref[:, cols:], tgt_ref[:, :cols])
        for i in range(1, n_mp):
            target_copy(i).start()
        target[...] = tgt_own[...]

    loads[3].wait()
    loads[4].wait()
    cosine, sine = cos_ref[...], sin_ref[...]
    kv = dot(tok_ref[...], wkv_ref[...])
    key = kv[:, :kv_dim]
    key = (key * cosine + pltpu.roll(key, HEAD_DIM // 2, 1) * sine).astype(bf16)
    value = kv[:, kv_dim:].astype(bf16)

    start = pl.multiple_of(me * own_tok, own_tok)
    cos_own = jnp.tile(cos_ref[pl.ds(start, own_tok), :], (n_pop, 1))
    sin_own = jnp.tile(sin_ref[pl.ds(start, own_tok), :], (n_pop, 1))
    token_of = start + lax.rem(lax.broadcasted_iota(jnp.int32, (rows, tok), 0), own_tok)
    causal = token_of >= lax.broadcasted_iota(jnp.int32, (rows, tok), 1)
    scale = HEAD_DIM ** (-0.5)

    from_all(0)
    from_all(1)

    def pop_at(r):
        r = lax.rem(r + 2 * n_pop, n_pop)
        return jnp.where(r < n_pop // 2, 2 * r, 2 * (n_pop - 1 - r) + 1)

    my_r = jnp.where(odd, n_pop - 1 - me // 2, me // 2)
    right, left = pop_at(my_r + 1), pop_at(my_r - 1)

    depth = n_pop // 2

    def hop(direction, step, g):
        at = pop_at(my_r - step if direction == 0 else my_r + step)
        return pltpu.make_async_remote_copy(
            src_ref=rings[g].at[at], dst_ref=rings[g].at[at],
            send_sem=ring_send.at[direction, step, g], recv_sem=ring_recv.at[direction, step, g],
            device_id={"pop": right if direction == 0 else left}, device_id_type=MESH,
        )

    def hops(direction, step, g):
        return step < depth - 1 or (step == depth - 1 and (2 * g >= many) == (direction == 1))

    def stacked(parts, *more):
        return jnp.concatenate(
            [p[i].astype(f32) for i in range(n_pop) for p in (parts,) + more], axis=0
        ).astype(bf16)

    pack_q = stacked(packs_q)
    ranks = n_pop * RANK
    eye = (
        lax.broadcasted_iota(jnp.int32, (ranks, ranks), 0)
        == lax.broadcasted_iota(jnp.int32, (ranks, ranks), 1)
    ).astype(bf16)
    low_rows = dot(stacked(packs_l), eye, ((0,), (0,)))[:own_tok]
    low_rows = jnp.tile(low_rows, (n_pop, 1))
    of_rank = lax.broadcasted_iota(jnp.int32, low_rows.shape, 1) // RANK
    of_row = lax.broadcasted_iota(jnp.int32, low_rows.shape, 0) // own_tok
    low_rows = jnp.where(of_rank == of_row, low_rows, 0.0).astype(bf16)
    for h in range(heads):
        lanes = slice(h * HEAD_DIM, (h + 1) * HEAD_DIM)
        g = [low <= lanes.start < high for low, high in groups].index(True)
        here = slice(lanes.start - groups[g][0], lanes.stop - groups[g][0])
        if here.start == 0:
            from_all(4 + g)
        parts = base_in[g]
        total = parts[0, :, here].astype(f32)
        for i in range(1, n_pop):
            total = total + parts[i, :, here].astype(f32)
        q = jnp.tile(total, (n_pop, 1)) + dot(low_rows, pack_q[:, lanes])
        q = (q * cos_own + pltpu.roll(q, HEAD_DIM // 2, 1) * sin_own).astype(bf16)
        s = dot(q, key, ((1,), (1,))) * scale
        s = jnp.where(causal, s, -1e30)
        e = jnp.exp(s - jnp.max(s, axis=1, keepdims=True))
        prob = (e / jnp.sum(e, axis=1, keepdims=True)).astype(bf16)
        mixed = dot(prob, value).astype(bf16)
        rings[g][me, :, here] = mixed
        if lanes.stop == groups[g][1]:
            for direction in range(2):
                hop(direction, 0, g).start()

    from_all(2)
    from_all(3)
    pack_a = stacked(packs_q, packs_o)
    pack_b = stacked(packs_b)
    pack_a_out[...] = pack_a
    pack_b_out[...] = pack_b
    loads[6].wait()

    def term_copy(at, block):
        return pltpu.make_async_remote_copy(
            src_ref=terms.at[at, block], dst_ref=terms_in.at[mc, at],
            send_sem=term_send.at[at, block], recv_sem=term_recv.at[mc, at],
            device_id={"mp": block}, device_id_type=MESH,
        )

    low_shape = (rows, n_pop * PACK)
    member_of = lax.broadcasted_iota(jnp.int32, low_shape, 0) // own_tok
    place = lax.broadcasted_iota(jnp.int32, low_shape, 1)
    keep = (place // PACK == member_of) & (lax.rem(place, PACK) >= RANK)

    def project(at):
        nt = ((1,), (1,))
        low = sum(
            dot(ring[at], pack_a[:, a:b], nt) for ring, (a, b) in zip(rings, groups)
        )
        low = jnp.where(keep, low, 0.0)
        y = sum(dot(ring[at], wo_ref[:, a:b], nt) for ring, (a, b) in zip(rings, groups))
        for piece in split3(low):
            y = y + dot(piece, pack_b)
        y = y.astype(bf16)
        for block in range(n_mp):
            terms[at, block] = y[block * per_mp:(block + 1) * per_mp]

            @pl.when(mc != block)
            def _():
                term_copy(at, block).start()

            @pl.when(mc == block)
            def _():
                terms_in[block, at] = terms[at, block]

    def squares(at, totals):
        for i in range(1, n_mp):
            source = lax.rem(mc + i, n_mp)
            pltpu.make_async_remote_copy(
                src_ref=terms.at[at, 0], dst_ref=terms_in.at[source, at],
                send_sem=term_send.at[at, 0], recv_sem=term_recv.at[source, at],
                device_id={"mp": source}, device_id_type=MESH,
            ).wait_recv()
        goal = target[pl.ds(pl.multiple_of(at * own_tok, own_tok), own_tok), :].astype(f32)
        result = []
        for k in range(members):
            span = slice(k * own_tok, (k + 1) * own_tok)
            out = terms_in[0, at, span].astype(f32)
            for c in range(1, n_mp):
                out = out + terms_in[c, at, span].astype(f32)
            diff = out - goal
            result.append(totals[k] + jnp.sum(diff * diff, axis=0, keepdims=True))
        return result

    project(me)

    @pl.when(mc != owner)
    def _():
        target_copy(1).wait_recv()

    totals = [jnp.zeros((1, cols), f32)] * members
    done = [me]
    for step in range(depth):
        for g in range(many):
            for direction in range(2):
                if hops(direction, step, g):
                    hop(direction, step, g).wait_recv()
                    if hops(direction, step + 1, g):
                        hop(direction, step + 1, g).start()
        landed = [pop_at(my_r - 1 - step)]
        if step < depth - 1:
            landed.append(pop_at(my_r + 1 + step))
        for at in landed:
            project(at)
        for at in done:
            totals = squares(at, totals)
        done = landed
    for at in done:
        totals = squares(at, totals)

    lane_row = lax.broadcasted_iota(jnp.int32, (1, 128), 1)
    mine = jnp.zeros((1, 128), f32)
    for k in range(members):
        value_k = jnp.sum(totals[k], axis=1, keepdims=True)
        mine = mine + jnp.where(lane_row == mc * members + k, value_k, 0.0)

    my_id = mc * n_pop + me
    errs[my_id] = mine

    def err_copy(i):
        other = lax.rem(my_id + i, n_dev)
        return pltpu.make_async_remote_copy(
            src_ref=errs.at[my_id], dst_ref=errs.at[my_id],
            send_sem=err_send.at[i], recv_sem=err_recv.at[i],
            device_id={"pop": lax.rem(other, n_pop), "mp": other // n_pop}, device_id_type=MESH,
        )

    def err_start(i, carry):
        err_copy(i).start()
        return carry

    def err_wait(i, carry):
        err_copy(i).wait_recv()
        return carry

    lax.fori_loop(1, n_dev, err_start, 0)
    for kind in range(4 + many):
        for i in range(1, n_pop):
            to_pop(i, kind).wait_send()
    for step in range(depth):
        for g in range(many):
            for direction in range(2):
                if hops(direction, step, g):
                    hop(direction, step, g).wait_send()
    for block in range(n_mp):
        @pl.when(mc != block)
        def _():
            for at in range(n_pop):
                term_copy(at, block).wait_send()

    @pl.when(mc == owner)
    def _():
        for i in range(1, n_mp):
            target_copy(i).wait_send()

    lax.fori_loop(1, n_dev, err_wait, 0)
    error = errs[0]
    for i in range(1, n_dev):
        error = error + errs[i]
    live = lane_row < n_pop
    fitness = -(error / (tok * width))
    mean = jnp.sum(jnp.where(live, fitness, 0.0), axis=1, keepdims=True) / n_pop
    dev = jnp.where(live, fitness - mean, 0.0)
    spread = jnp.sum(dev * dev, axis=1, keepdims=True) / n_pop
    weight = dev / jnp.sqrt(spread + spread_floor)
    stat_out[...] = jnp.concatenate(
        [fitness, weight, jnp.zeros((6, 128), f32)], axis=0
    )

    def err_drain(i, carry):
        err_copy(i).wait_send()
        return carry

    lax.fori_loop(1, n_dev, err_drain, 0)


def grad_kernel(a_ref, b_ref, stat_ref, gq_hbm, got_hbm, fit_ref, gq_ref, got_ref, sem):
    pack_a = a_ref[...]
    pack_b = b_ref[...].astype(f32)
    rows, cols = pack_b.shape
    row = lax.broadcasted_iota(jnp.int32, (rows, 128), 0)
    lane = lax.broadcasted_iota(jnp.int32, (rows, 128), 1)
    per_row = jnp.sum(jnp.where(lane == row // PACK, stat_ref[1:2, :], 0.0), axis=1, keepdims=True)
    per_row = per_row / (noise_scale * noise_scale)
    kind = lax.rem(lax.broadcasted_iota(jnp.int32, (rows, 1), 0), PACK)
    edges = (0, (cols // 2 + 127) // 128 * 128, cols)
    copies = []
    for out, target, weight in (
        (gq_ref, gq_hbm, jnp.where(kind < RANK, per_row, 0.0)),
        (got_ref, got_hbm, jnp.where(kind >= RANK, per_row, 0.0)),
    ):
        pieces = jnp.concatenate(split3(pack_b * weight), axis=0)
        right = jnp.concatenate([pack_a] * 3, axis=0)
        for low, high in zip(edges[:-1], edges[1:]):
            out[low:high, :] = dot(pieces[:, low:high], right, ((0,), (0,)))
            copy = pltpu.make_async_copy(
                out.at[low:high], target.at[low:high], sem.at[len(copies)]
            )
            copy.start()
            copies.append(copy)
    me = lax.axis_index("pop")
    fit_ref[0] = jnp.sum(jnp.where(lane[:1] == me, stat_ref[0:1, :], 0.0))
    for copy in copies:
        copy.wait()


def per_device_fast(
    n_pop, n_mp,
    tokens, target, w_query, w_key, w_value, w_out,
    query_left_factors, query_right_factors, o_left, o_right, member_ids,
):
    tok, width = tokens.shape
    feats = w_query.shape[1]
    cols = w_out.shape[1]
    own_tok = tok // n_pop
    rows = n_pop * own_tok
    cosine, sine = rope_tables(tok, HEAD_DIM)
    vmem = pl.BlockSpec(memory_space=pltpu.VMEM)
    hbm = pl.BlockSpec(memory_space=pltpu.HBM)
    smem = pl.BlockSpec(memory_space=pltpu.SMEM)
    dma = pltpu.SemaphoreType.DMA
    depth = n_pop // 2
    n_dev = n_pop * n_mp
    widths = [high - low for low, high in head_groups(feats)]
    like = lambda x: pltpu.VMEM(x.shape, x.dtype)
    wot = w_out.T
    pack_a, pack_b, stat = pl.pallas_call(
        functools.partial(forward_kernel, n_pop, n_mp, width),
        name="forward",
        out_shape=(
            jax.ShapeDtypeStruct((n_pop * PACK, feats), bf16),
            jax.ShapeDtypeStruct((n_pop * PACK, cols), bf16),
            jax.ShapeDtypeStruct((8, 128), f32),
        ),
        in_specs=[hbm] * 6 + [vmem] * 4 + [smem] + [vmem] * 2,
        out_specs=(vmem, vmem, vmem),
        scratch_shapes=[
            like(tokens), pltpu.VMEM((tok, 2 * cols), bf16), like(w_query),
            pltpu.VMEM((w_key.shape[0], 2 * w_key.shape[1]), bf16), like(wot), like(target),
            *(pltpu.VMEM((n_pop, own_tok, w), LINK) for w in widths),
            *(pltpu.VMEM((n_pop, own_tok, w), LINK) for w in widths),
            *(pltpu.VMEM((n_pop, rows, w), bf16) for w in widths),
            pltpu.VMEM((n_pop, RANK, 128), bf16),
            pltpu.VMEM((n_pop, RANK, 128), bf16),
            pltpu.VMEM((RANK, feats), bf16),
            pltpu.VMEM((n_pop, RANK, feats), bf16),
            pltpu.VMEM((RANK, feats), bf16),
            pltpu.VMEM((n_pop, RANK, feats), bf16),
            pltpu.VMEM((n_pop, PACK, cols), bf16),
            pltpu.VMEM((n_pop, PACK, cols), bf16),
            pltpu.VMEM((n_pop, n_mp, rows // n_mp, cols), bf16),
            pltpu.VMEM((n_mp, n_pop, rows // n_mp, cols), bf16),
            pltpu.VMEM((tok, cols), bf16),
            pltpu.VMEM((tok, cols), bf16),
            pltpu.VMEM((n_dev, 1, 128), f32),
            dma((7,)),
            dma((4 + len(widths), n_pop)), dma((4 + len(widths), n_pop)),
            dma((2, depth, len(widths))), dma((2, depth, len(widths))),
            dma((n_pop, n_mp)), dma((n_mp, n_pop)),
            dma((n_mp,)), dma,
            dma((n_dev,)), dma((n_dev,)),
        ],
        compiler_params=pltpu.CompilerParams(
            collective_id=0, has_side_effects=True, vmem_limit_bytes=60 * 1024 * 1024
        ),
    )(tokens, w_query, w_key, w_value, wot, target,
      query_left_factors[0].T, query_right_factors[0], o_left[0].T, o_right[0], member_ids,
      jnp.asarray(cosine), jnp.asarray(sine))
    grad = jax.ShapeDtypeStruct((cols, feats), f32)
    grad_query, grad_out_t, fitness = pl.pallas_call(
        grad_kernel,
        name="grads",
        out_shape=(grad, grad, jax.ShapeDtypeStruct((1,), f32)),
        in_specs=[vmem, vmem, vmem],
        out_specs=(hbm, hbm, smem),
        scratch_shapes=[like(grad), like(grad), dma((4,))],
    )(pack_a, pack_b, stat)
    return grad_query, grad_out_t.T, fitness


def tables(count, head_size):
    position = jnp.arange(count, dtype=jnp.float32)
    index = jnp.arange(head_size // 2, dtype=jnp.float32)
    freq = jnp.exp(-math.log(rope_base) * 2.0 * index / head_size)
    angle = position[:, None] * freq[None, :]
    return (jnp.cos(angle)[:, None, :], jnp.sin(angle)[:, None, :])


def rotate(field, cosine_table, sine):
    half = field.shape[-1] // 2
    first = field[..., :half]
    second = field[..., half:]
    return jnp.concatenate(
        [first * cosine_table - second * sine, second * cosine_table + first * sine], axis=-1
    )


def per_device(
    tokens,
    target,
    w_query,
    w_key,
    w_value,
    w_out,
    query_left_factors,
    query_right_factors,
    o_left,
    o_right,
    member_ids,
):
    tok = tokens.shape[0]
    local_feats = w_query.shape[1]
    local_kv = w_key.shape[1] // HEAD_DIM
    group = group_of(w_query, w_key)
    local_heads = local_kv * group
    slots = query_left_factors.shape[0]
    scale = HEAD_DIM ** (-0.5)
    cosine_table, sine = tables(tok, HEAD_DIM)
    base = jnp.dot(
        tokens,
        lax.all_gather(w_query, "pop", axis=0, tiled=True),
        preferred_element_type=jnp.float32,
    )
    keys = rotate(
        jnp.dot(tokens, w_key, preferred_element_type=jnp.float32).reshape(tok, local_kv, HEAD_DIM),
        cosine_table,
        sine,
    ).astype(jnp.bfloat16)
    values = (
        jnp.dot(tokens, w_value, preferred_element_type=jnp.float32)
        .astype(jnp.bfloat16)
        .reshape(tok, local_kv, HEAD_DIM)
    )
    signs = (1 - 2 * (member_ids % 2)).astype(jnp.float32)
    factor = noise_scale * signs[:, None, None]
    lowrank_product = jnp.einsum(
        "td,mdr->mtr", tokens, query_left_factors, preferred_element_type=jnp.float32
    ).astype(jnp.bfloat16)
    query = base[None] + factor * jnp.einsum(
        "olj,ojv->olv", lowrank_product, query_right_factors, preferred_element_type=jnp.float32
    )
    query = rotate(
        query.reshape(slots, tok, local_heads, HEAD_DIM), cosine_table[None], sine[None]
    ).astype(jnp.bfloat16)
    query = query.reshape(slots, tok, local_kv, group, HEAD_DIM)
    scores = jnp.einsum("mtkgd,skd->mkgts", query, keys, preferred_element_type=jnp.float32) * scale
    causal = jnp.arange(tok)[:, None] >= jnp.arange(tok)[None, :]
    scores = jnp.where(causal, scores, -1e30)
    probs = jax.nn.softmax(scores, axis=-1).astype(jnp.bfloat16)
    mixed = (
        jnp.einsum("mkgts,skd->mtkgd", probs, values, preferred_element_type=jnp.float32)
        .astype(jnp.bfloat16)
        .reshape(slots, tok, local_feats)
    )
    low_out = jnp.einsum("mtf,mfr->mtr", mixed, o_left, preferred_element_type=jnp.float32)
    right_full = o_right.astype(jnp.float32)
    part = jnp.einsum(
        "mtf,fe->mte",
        mixed,
        lax.all_gather(w_out, "pop", axis=1, tiled=True),
        preferred_element_type=jnp.float32,
    )
    term = part + factor * jnp.einsum(
        "mtr,mre->mte", low_out, right_full, precision=lax.Precision.HIGHEST
    )
    output = lax.psum_scatter(
        term.astype(jnp.bfloat16), "mp", scatter_dimension=2, tiled=True
    ).astype(jnp.float32)
    diff = output - target.astype(jnp.float32)[None]
    errors = lax.psum(jnp.sum(diff * diff, axis=(1, 2)), "mp")
    fitness = -(errors / (tok * tokens.shape[1]))
    count = slots * lax.axis_size("pop")
    mean = lax.psum(jnp.sum(fitness), "pop") / count
    spread = lax.psum(jnp.sum((fitness - mean) * (fitness - mean)), "pop") / count
    weight = signs * (fitness - mean) / jnp.sqrt(spread + spread_floor)
    every_weight = lax.all_gather(weight, "pop", axis=0, tiled=True)
    right_factors_gathered, left_all = (
        lax.all_gather(query_right_factors, "pop", axis=0, tiled=True),
        lax.all_gather(o_left, "pop", axis=0, tiled=True),
    )
    rows_q = lax.all_to_all(query_left_factors, "pop", split_axis=1, concat_axis=0, tiled=True)
    cols_o = lax.all_to_all(o_right, "pop", split_axis=2, concat_axis=0, tiled=True)
    whole_population = rows_q.shape[0]
    left_q = jnp.transpose(
        rows_q.astype(jnp.float32) * every_weight[:, None, None], (1, 0, 2)
    ).reshape(rows_q.shape[1], whole_population * RANK)
    right_q = right_factors_gathered.astype(jnp.float32).reshape(
        whole_population * RANK, local_feats
    )
    grad_query = jnp.dot(left_q, right_q, precision=lax.Precision.HIGHEST) / noise_scale
    output_left_factor = jnp.transpose(
        left_all.astype(jnp.float32) * every_weight[:, None, None], (1, 0, 2)
    ).reshape(local_feats, whole_population * RANK)
    right_o = cols_o.astype(jnp.float32).reshape(whole_population * RANK, cols_o.shape[2])
    grad_out = jnp.dot(output_left_factor, right_o, precision=lax.Precision.HIGHEST) / noise_scale
    return (grad_query, grad_out, fitness)


def group_of(w_query, w_key):
    return w_query.shape[1] // w_key.shape[1]


def pick(args, n_pop, n_mp):
    tok = args[0].shape[0]
    kernel = (
        args[6].shape[0] == n_pop
        and n_pop % n_mp == 0
        and n_pop % 2 == 0
        and n_pop * PACK <= 128
        and tok % (n_pop * 16) == 0
        and tok // n_pop < 128
        and args[2].shape[1] // n_mp == 2 * args[5].shape[1] // n_pop
        and args[2].shape[0] == args[5].shape[1]
        and args[3].shape[1] == n_mp * HEAD_DIM
    )
    return functools.partial(per_device_fast, n_pop, n_mp) if kernel else per_device


def solution(mesh):
    placed = (
        P(),
        P(None, "mp"),
        P("pop", "mp"),
        P(None, "mp"),
        P(None, "mp"),
        P("mp", "pop"),
        P("pop", None, None),
        P("pop", None, "mp"),
        P("pop", "mp", None),
        P("pop", None, None),
        P("pop"),
    )
    n_pop, n_mp = mesh.shape["pop"], mesh.shape["mp"]

    def whole(*args):
        return jax.shard_map(
            pick(args, n_pop, n_mp),
            mesh=mesh,
            in_specs=placed,
            out_specs=(P("pop", "mp"), P("mp", "pop"), P("pop")),
            check_vma=False,
        )(*args)

    return whole
```

```python
import functools
import math

import jax
import jax.numpy as jnp
import numpy as np
from jax import lax
from jax.experimental import pallas as pl
from jax.experimental.pallas import tpu as pltpu
from jax.sharding import PartitionSpec as P

HEAD_DIM = 128
RANK = 4
PACK = 8
LINK = jnp.bfloat16

noise_scale = 0.5
rope_base = 1000000.0
spread_floor = 0.001
MESH = pl.DeviceIdType.MESH
f32 = jnp.float32
bf16 = jnp.bfloat16


def rope_tables(count, head_size):
    index = np.arange(head_size // 2, dtype=np.float64)
    freq = np.exp(-math.log(rope_base) * 2.0 * index / head_size)
    angle = np.arange(count, dtype=np.float64)[:, None] * freq[None, :]
    cosine, sine = np.cos(angle), np.sin(angle)
    return (
        np.concatenate([cosine, cosine], 1).astype(np.float32),
        np.concatenate([-sine, sine], 1).astype(np.float32),
    )


def head_groups(feats):
    heads = feats // HEAD_DIM
    return [(h * HEAD_DIM, min(h + 4, heads) * HEAD_DIM) for h in range(0, heads, 4)]


def dot(a, b, dims=((1,), (0,))):
    return lax.dot_general(a, b, (dims, ((), ())), preferred_element_type=f32)


def split3(x):
    hi = x.astype(bf16)
    rest = x - hi.astype(f32)
    mid = rest.astype(bf16)
    low = (rest - mid.astype(f32)).astype(bf16)
    return hi, mid, low


def forward_kernel(
    n_pop, n_mp, width,
    tok_hbm, wq_hbm, wk_hbm, wv_hbm, wo_hbm, tgt_hbm, ql_ref, qr_ref, ol_ref, or_ref, id_ref,
    cos_ref, sin_ref,
    pack_a_out, pack_b_out, stat_out,
    *refs,
):
    groups = head_groups(wq_hbm.shape[1])
    many = len(groups)
    tok_ref, window_ref, wq_ref, wkv_ref, wo_ref, tgt_ref = refs[:6]
    refs = refs[6:]
    mine_base, base_in, rings = refs[:many], refs[many:2 * many], refs[2 * many:3 * many]
    (
        mine_l, packs_l, mine_q, packs_q, mine_o, packs_o, mine_b, packs_b,
        terms, terms_in, tgt_own, target, errs, load_sem, pop_send, pop_recv,
        ring_send, ring_recv, term_send, term_recv, tgt_send, tgt_recv, err_send, err_recv,
    ) = refs[3 * many:]
    me = lax.axis_index("pop")
    mc = lax.axis_index("mp")
    n_dev = n_pop * n_mp
    tok, feats = tok_ref.shape[0], wq_ref.shape[1]
    own_tok = tok // n_pop
    rows = n_pop * own_tok
    per_mp = rows // n_mp
    heads = feats // HEAD_DIM
    cols = wo_ref.shape[0]
    members = n_pop // n_mp
    odd = lax.rem(me, 2) == 1

    kv_dim = wk_hbm.shape[1]
    around = pl.ds(pl.multiple_of(me // 2 * 2 * cols, 128), 2 * cols)
    loads = [
        pltpu.make_async_copy(src, dst, load_sem.at[i])
        for i, (src, dst) in enumerate((
            (wq_hbm, wq_ref), (tok_hbm.at[:, around], window_ref), (tok_hbm, tok_ref),
            (wk_hbm, wkv_ref.at[:, :kv_dim]), (wv_hbm, wkv_ref.at[:, kv_dim:]),
            (tgt_hbm, tgt_ref), (wo_hbm, wo_ref),
        ))
    ]
    for load in loads:
        load.start()

    barrier = pltpu.get_barrier_semaphore()

    def greet(i, carry):
        other = lax.rem(mc * n_pop + me + i, n_dev)
        pl.semaphore_signal(
            barrier, inc=1,
            device_id={"pop": lax.rem(other, n_pop), "mp": other // n_pop},
            device_id_type=MESH,
        )
        return carry

    lax.fori_loop(1, n_dev, greet, 0)

    sign = 1 - 2 * lax.rem(id_ref[0], 2)
    factor = noise_scale * sign.astype(f32)
    loads[0].wait()
    loads[1].wait()
    window = window_ref[...]
    wq = wq_ref[...]
    first, second = window[:, :cols], window[:, cols:]
    base = dot(jnp.where(odd, second, first), wq)
    for mine, (low, high) in zip(mine_base, groups):
        mine[...] = base[:, low:high].reshape(mine.shape).astype(LINK)
    mine_q[...] = (qr_ref[...].astype(f32) * factor).astype(bf16)

    pl.semaphore_wait(barrier, n_dev - 1)

    def to_pop(i, kind):
        other = lax.rem(me + i, n_pop)
        src, dst = (
            (mine_q, packs_q),
            (mine_l.at[other], packs_l),
            (mine_o, packs_o),
            (mine_b.at[other], packs_b),
            *((mine.at[other], landing) for mine, landing in zip(mine_base, base_in)),
        )[kind]
        return pltpu.make_async_remote_copy(
            src_ref=src, dst_ref=dst.at[me], send_sem=pop_send.at[kind, i],
            recv_sem=pop_recv.at[kind, i], device_id={"pop": other}, device_id_type=MESH,
        )

    def to_all(kind):
        for i in range(1, n_pop):
            to_pop(i, kind).start()

    def from_all(kind):
        for i in range(1, n_pop):
            to_pop(i, kind).wait_recv()

    to_all(4)
    to_all(0)
    loads[2].wait()
    ql = ql_ref[...]
    low = dot(ql, tok_ref[...], ((1,), (1,))).astype(bf16).astype(f32)
    for q in range(n_pop):
        mine_l[q] = jnp.concatenate(
            [low[:, q * own_tok:(q + 1) * own_tok], jnp.zeros((RANK, 128 - own_tok), f32)], axis=1
        ).astype(bf16)
    to_all(1)
    for g in range(1, many):
        to_all(4 + g)
    mine_o[...] = ol_ref[...]
    both = jnp.concatenate([ql.astype(f32), or_ref[...].astype(f32) * factor], axis=0)
    for q in range(n_pop):
        mine_b[q] = both[:, q * cols:(q + 1) * cols].astype(bf16)
    to_all(2)
    to_all(3)
    for mine, packs in (*zip(mine_base, base_in), (mine_l, packs_l), (mine_b, packs_b)):
        packs[me] = mine[me]
    packs_q[me] = mine_q[...]
    packs_o[me] = mine_o[...]

    owner = me // (n_pop // n_mp)

    def target_copy(i):
        return pltpu.make_async_remote_copy(
            src_ref=tgt_own, dst_ref=target, send_sem=tgt_send.at[i], recv_sem=tgt_recv,
            device_id={"mp": lax.rem(mc + i, n_mp)}, device_id_type=MESH,
        )

    loads[5].wait()

    @pl.when(mc == owner)
    def _():
        tgt_own[...] = jnp.where(odd, tgt_ref[:, cols:], tgt_ref[:, :cols])
        for i in range(1, n_mp):
            target_copy(i).start()
        target[...] = tgt_own[...]

    loads[3].wait()
    loads[4].wait()
    cosine, sine = cos_ref[...], sin_ref[...]
    kv = dot(tok_ref[...], wkv_ref[...])
    key = kv[:, :kv_dim]
    key = (key * cosine + pltpu.roll(key, HEAD_DIM // 2, 1) * sine).astype(bf16)
    value = kv[:, kv_dim:].astype(bf16)

    start = pl.multiple_of(me * own_tok, own_tok)
    cos_own = jnp.tile(cos_ref[pl.ds(start, own_tok), :], (n_pop, 1))
    sin_own = jnp.tile(sin_ref[pl.ds(start, own_tok), :], (n_pop, 1))
    token_of = start + lax.rem(lax.broadcasted_iota(jnp.int32, (rows, tok), 0), own_tok)
    causal = token_of >= lax.broadcasted_iota(jnp.int32, (rows, tok), 1)
    scale = HEAD_DIM ** (-0.5)

    from_all(0)
    from_all(1)

    def pop_at(r):
        r = lax.rem(r + 2 * n_pop, n_pop)
        return jnp.where(r < n_pop // 2, 2 * r, 2 * (n_pop - 1 - r) + 1)

    my_r = jnp.where(odd, n_pop - 1 - me // 2, me // 2)
    right, left = pop_at(my_r + 1), pop_at(my_r - 1)

    depth = n_pop // 2

    def hop(direction, step, g):
        at = pop_at(my_r - step if direction == 0 else my_r + step)
        return pltpu.make_async_remote_copy(
            src_ref=rings[g].at[at], dst_ref=rings[g].at[at],
            send_sem=ring_send.at[direction, step, g], recv_sem=ring_recv.at[direction, step, g],
            device_id={"pop": right if direction == 0 else left}, device_id_type=MESH,
        )

    def hops(direction, step, g):
        return step < depth - 1 or (step == depth - 1 and (2 * g >= many) == (direction == 1))

    def stacked(parts, *more):
        return jnp.concatenate(
            [p[i].astype(f32) for i in range(n_pop) for p in (parts,) + more], axis=0
        ).astype(bf16)

    pack_q = stacked(packs_q)
    ranks = n_pop * RANK
    eye = (
        lax.broadcasted_iota(jnp.int32, (ranks, ranks), 0)
        == lax.broadcasted_iota(jnp.int32, (ranks, ranks), 1)
    ).astype(bf16)
    low_rows = dot(stacked(packs_l), eye, ((0,), (0,)))[:own_tok]
    low_rows = jnp.tile(low_rows, (n_pop, 1))
    of_rank = lax.broadcasted_iota(jnp.int32, low_rows.shape, 1) // RANK
    of_row = lax.broadcasted_iota(jnp.int32, low_rows.shape, 0) // own_tok
    low_rows = jnp.where(of_rank == of_row, low_rows, 0.0).astype(bf16)
    for h in range(heads):
        lanes = slice(h * HEAD_DIM, (h + 1) * HEAD_DIM)
        g = [low <= lanes.start < high for low, high in groups].index(True)
        here = slice(lanes.start - groups[g][0], lanes.stop - groups[g][0])
        if here.start == 0:
            from_all(4 + g)
        parts = base_in[g]
        total = parts[0, :, here].astype(f32)
        for i in range(1, n_pop):
            total = total + parts[i, :, here].astype(f32)
        q = jnp.tile(total, (n_pop, 1)) + dot(low_rows, pack_q[:, lanes])
        q = (q * cos_own + pltpu.roll(q, HEAD_DIM // 2, 1) * sin_own).astype(bf16)
        s = dot(q, key, ((1,), (1,))) * scale
        s = jnp.where(causal, s, -1e30)
        e = jnp.exp(s - jnp.max(s, axis=1, keepdims=True))
        prob = (e / jnp.sum(e, axis=1, keepdims=True)).astype(bf16)
        mixed = dot(prob, value).astype(bf16)
        rings[g][me, :, here] = mixed
        if lanes.stop == groups[g][1]:
            for direction in range(2):
                hop(direction, 0, g).start()

    from_all(2)
    from_all(3)
    pack_a = stacked(packs_q, packs_o)
    pack_b = stacked(packs_b)
    pack_a_out[...] = pack_a
    pack_b_out[...] = pack_b
    loads[6].wait()

    def term_copy(at, block):
        return pltpu.make_async_remote_copy(
            src_ref=terms.at[at, block], dst_ref=terms_in.at[mc, at],
            send_sem=term_send.at[at, block], recv_sem=term_recv.at[mc, at],
            device_id={"mp": block}, device_id_type=MESH,
        )

    low_shape = (rows, n_pop * PACK)
    member_of = lax.broadcasted_iota(jnp.int32, low_shape, 0) // own_tok
    place = lax.broadcasted_iota(jnp.int32, low_shape, 1)
    keep = (place // PACK == member_of) & (lax.rem(place, PACK) >= RANK)

    def project(at):
        nt = ((1,), (1,))
        low = sum(
            dot(ring[at], pack_a[:, a:b], nt) for ring, (a, b) in zip(rings, groups)
        )
        low = jnp.where(keep, low, 0.0)
        y = sum(dot(ring[at], wo_ref[:, a:b], nt) for ring, (a, b) in zip(rings, groups))
        for piece in split3(low):
            y = y + dot(piece, pack_b)
        y = y.astype(bf16)
        for block in range(n_mp):
            terms[at, block] = y[block * per_mp:(block + 1) * per_mp]

            @pl.when(mc != block)
            def _():
                term_copy(at, block).start()

            @pl.when(mc == block)
            def _():
                terms_in[block, at] = terms[at, block]

    def squares(at, totals):
        for i in range(1, n_mp):
            source = lax.rem(mc + i, n_mp)
            pltpu.make_async_remote_copy(
                src_ref=terms.at[at, 0], dst_ref=terms_in.at[source, at],
                send_sem=term_send.at[at, 0], recv_sem=term_recv.at[source, at],
                device_id={"mp": source}, device_id_type=MESH,
            ).wait_recv()
        goal = target[pl.ds(pl.multiple_of(at * own_tok, own_tok), own_tok), :].astype(f32)
        result = []
        for k in range(members):
            span = slice(k * own_tok, (k + 1) * own_tok)
            out = terms_in[0, at, span].astype(f32)
            for c in range(1, n_mp):
                out = out + terms_in[c, at, span].astype(f32)
            diff = out - goal
            result.append(totals[k] + jnp.sum(diff * diff, axis=0, keepdims=True))
        return result

    project(me)

    @pl.when(mc != owner)
    def _():
        target_copy(1).wait_recv()

    totals = [jnp.zeros((1, cols), f32)] * members
    done = [me]
    for step in range(depth):
        for g in range(many):
            for direction in range(2):
                if hops(direction, step, g):
                    hop(direction, step, g).wait_recv()
                    if hops(direction, step + 1, g):
                        hop(direction, step + 1, g).start()
        landed = [pop_at(my_r - 1 - step)]
        if step < depth - 1:
            landed.append(pop_at(my_r + 1 + step))
        for at in landed:
            project(at)
        for at in done:
            totals = squares(at, totals)
        done = landed
    for at in done:
        totals = squares(at, totals)

    lane_row = lax.broadcasted_iota(jnp.int32, (1, 128), 1)
    mine = jnp.zeros((1, 128), f32)
    for k in range(members):
        value_k = jnp.sum(totals[k], axis=1, keepdims=True)
        mine = mine + jnp.where(lane_row == mc * members + k, value_k, 0.0)

    my_id = mc * n_pop + me
    errs[my_id] = mine

    def err_copy(i):
        other = lax.rem(my_id + i, n_dev)
        return pltpu.make_async_remote_copy(
            src_ref=errs.at[my_id], dst_ref=errs.at[my_id],
            send_sem=err_send.at[i], recv_sem=err_recv.at[i],
            device_id={"pop": lax.rem(other, n_pop), "mp": other // n_pop}, device_id_type=MESH,
        )

    def err_start(i, carry):
        err_copy(i).start()
        return carry

    def err_wait(i, carry):
        err_copy(i).wait_recv()
        return carry

    lax.fori_loop(1, n_dev, err_start, 0)
    for kind in range(4 + many):
        for i in range(1, n_pop):
            to_pop(i, kind).wait_send()
    for step in range(depth):
        for g in range(many):
            for direction in range(2):
                if hops(direction, step, g):
                    hop(direction, step, g).wait_send()
    for block in range(n_mp):
        @pl.when(mc != block)
        def _():
            for at in range(n_pop):
                term_copy(at, block).wait_send()

    @pl.when(mc == owner)
    def _():
        for i in range(1, n_mp):
            target_copy(i).wait_send()

    lax.fori_loop(1, n_dev, err_wait, 0)
    error = errs[0]
    for i in range(1, n_dev):
        error = error + errs[i]
    live = lane_row < n_pop
    fitness = -(error / (tok * width))
    mean = jnp.sum(jnp.where(live, fitness, 0.0), axis=1, keepdims=True) / n_pop
    dev = jnp.where(live, fitness - mean, 0.0)
    spread = jnp.sum(dev * dev, axis=1, keepdims=True) / n_pop
    weight = dev / jnp.sqrt(spread + spread_floor)
    stat_out[...] = jnp.concatenate(
        [fitness, weight, jnp.zeros((6, 128), f32)], axis=0
    )

    def err_drain(i, carry):
        err_copy(i).wait_send()
        return carry

    lax.fori_loop(1, n_dev, err_drain, 0)


def grad_kernel(a_ref, b_ref, stat_ref, gq_hbm, got_hbm, fit_ref, gq_ref, got_ref, sem):
    pack_a = a_ref[...]
    pack_b = b_ref[...].astype(f32)
    rows, cols = pack_b.shape
    row = lax.broadcasted_iota(jnp.int32, (rows, 128), 0)
    lane = lax.broadcasted_iota(jnp.int32, (rows, 128), 1)
    per_row = jnp.sum(jnp.where(lane == row // PACK, stat_ref[1:2, :], 0.0), axis=1, keepdims=True)
    per_row = per_row / (noise_scale * noise_scale)
    kind = lax.rem(lax.broadcasted_iota(jnp.int32, (rows, 1), 0), PACK)
    edges = (0, (cols // 2 + 127) // 128 * 128, cols)
    copies = []
    for out, target, weight in (
        (gq_ref, gq_hbm, jnp.where(kind < RANK, per_row, 0.0)),
        (got_ref, got_hbm, jnp.where(kind >= RANK, per_row, 0.0)),
    ):
        pieces = jnp.concatenate(split3(pack_b * weight), axis=0)
        right = jnp.concatenate([pack_a] * 3, axis=0)
        for low, high in zip(edges[:-1], edges[1:]):
            out[low:high, :] = dot(pieces[:, low:high], right, ((0,), (0,)))
            copy = pltpu.make_async_copy(
                out.at[low:high], target.at[low:high], sem.at[len(copies)]
            )
            copy.start()
            copies.append(copy)
    me = lax.axis_index("pop")
    fit_ref[0] = jnp.sum(jnp.where(lane[:1] == me, stat_ref[0:1, :], 0.0))
    for copy in copies:
        copy.wait()


def per_device_fast(
    n_pop, n_mp,
    tokens, target, w_query, w_key, w_value, w_out,
    query_left_factors, query_right_factors, o_left, o_right, member_ids,
):
    tok, width = tokens.shape
    feats = w_query.shape[1]
    cols = w_out.shape[1]
    own_tok = tok // n_pop
    rows = n_pop * own_tok
    cosine, sine = rope_tables(tok, HEAD_DIM)
    vmem = pl.BlockSpec(memory_space=pltpu.VMEM)
    hbm = pl.BlockSpec(memory_space=pltpu.HBM)
    smem = pl.BlockSpec(memory_space=pltpu.SMEM)
    dma = pltpu.SemaphoreType.DMA
    depth = n_pop // 2
    n_dev = n_pop * n_mp
    widths = [high - low for low, high in head_groups(feats)]
    like = lambda x: pltpu.VMEM(x.shape, x.dtype)
    wot = w_out.T
    pack_a, pack_b, stat = pl.pallas_call(
        functools.partial(forward_kernel, n_pop, n_mp, width),
        name="forward",
        out_shape=(
            jax.ShapeDtypeStruct((n_pop * PACK, feats), bf16),
            jax.ShapeDtypeStruct((n_pop * PACK, cols), bf16),
            jax.ShapeDtypeStruct((8, 128), f32),
        ),
        in_specs=[hbm] * 6 + [vmem] * 4 + [smem] + [vmem] * 2,
        out_specs=(vmem, vmem, vmem),
        scratch_shapes=[
            like(tokens), pltpu.VMEM((tok, 2 * cols), bf16), like(w_query),
            pltpu.VMEM((w_key.shape[0], 2 * w_key.shape[1]), bf16), like(wot), like(target),
            *(pltpu.VMEM((n_pop, own_tok, w), LINK) for w in widths),
            *(pltpu.VMEM((n_pop, own_tok, w), LINK) for w in widths),
            *(pltpu.VMEM((n_pop, rows, w), bf16) for w in widths),
            pltpu.VMEM((n_pop, RANK, 128), bf16),
            pltpu.VMEM((n_pop, RANK, 128), bf16),
            pltpu.VMEM((RANK, feats), bf16),
            pltpu.VMEM((n_pop, RANK, feats), bf16),
            pltpu.VMEM((RANK, feats), bf16),
            pltpu.VMEM((n_pop, RANK, feats), bf16),
            pltpu.VMEM((n_pop, PACK, cols), bf16),
            pltpu.VMEM((n_pop, PACK, cols), bf16),
            pltpu.VMEM((n_pop, n_mp, rows // n_mp, cols), bf16),
            pltpu.VMEM((n_mp, n_pop, rows // n_mp, cols), bf16),
            pltpu.VMEM((tok, cols), bf16),
            pltpu.VMEM((tok, cols), bf16),
            pltpu.VMEM((n_dev, 1, 128), f32),
            dma((7,)),
            dma((4 + len(widths), n_pop)), dma((4 + len(widths), n_pop)),
            dma((2, depth, len(widths))), dma((2, depth, len(widths))),
            dma((n_pop, n_mp)), dma((n_mp, n_pop)),
            dma((n_mp,)), dma,
            dma((n_dev,)), dma((n_dev,)),
        ],
        compiler_params=pltpu.CompilerParams(
            collective_id=0, has_side_effects=True, vmem_limit_bytes=60 * 1024 * 1024
        ),
    )(tokens, w_query, w_key, w_value, wot, target,
      query_left_factors[0].T, query_right_factors[0], o_left[0].T, o_right[0], member_ids,
      jnp.asarray(cosine), jnp.asarray(sine))
    grad = jax.ShapeDtypeStruct((cols, feats), f32)
    grad_query, grad_out_t, fitness = pl.pallas_call(
        grad_kernel,
        name="grads",
        out_shape=(grad, grad, jax.ShapeDtypeStruct((1,), f32)),
        in_specs=[vmem, vmem, vmem],
        out_specs=(hbm, hbm, smem),
        scratch_shapes=[like(grad), like(grad), dma((4,))],
    )(pack_a, pack_b, stat)
    return grad_query, grad_out_t.T, fitness


def tables(count, head_size):
    position = jnp.arange(count, dtype=jnp.float32)
    index = jnp.arange(head_size // 2, dtype=jnp.float32)
    freq = jnp.exp(-math.log(rope_base) * 2.0 * index / head_size)
    angle = position[:, None] * freq[None, :]
    return (jnp.cos(angle)[:, None, :], jnp.sin(angle)[:, None, :])


def rotate(field, cosine_table, sine):
    half = field.shape[-1] // 2
    first = field[..., :half]
    second = field[..., half:]
    return jnp.concatenate(
        [first * cosine_table - second * sine, second * cosine_table + first * sine], axis=-1
    )


def per_device(
    tokens,
    target,
    w_query,
    w_key,
    w_value,
    w_out,
    query_left_factors,
    query_right_factors,
    o_left,
    o_right,
    member_ids,
):
    tok = tokens.shape[0]
    local_feats = w_query.shape[1]
    local_kv = w_key.shape[1] // HEAD_DIM
    group = group_of(w_query, w_key)
    local_heads = local_kv * group
    slots = query_left_factors.shape[0]
    scale = HEAD_DIM ** (-0.5)
    cosine_table, sine = tables(tok, HEAD_DIM)
    base = jnp.dot(
        tokens,
        lax.all_gather(w_query, "pop", axis=0, tiled=True),
        preferred_element_type=jnp.float32,
    )
    keys = rotate(
        jnp.dot(tokens, w_key, preferred_element_type=jnp.float32).reshape(tok, local_kv, HEAD_DIM),
        cosine_table,
        sine,
    ).astype(jnp.bfloat16)
    values = (
        jnp.dot(tokens, w_value, preferred_element_type=jnp.float32)
        .astype(jnp.bfloat16)
        .reshape(tok, local_kv, HEAD_DIM)
    )
    signs = (1 - 2 * (member_ids % 2)).astype(jnp.float32)
    factor = noise_scale * signs[:, None, None]
    lowrank_product = jnp.einsum(
        "td,mdr->mtr", tokens, query_left_factors, preferred_element_type=jnp.float32
    ).astype(jnp.bfloat16)
    query = base[None] + factor * jnp.einsum(
        "olj,ojv->olv", lowrank_product, query_right_factors, preferred_element_type=jnp.float32
    )
    query = rotate(
        query.reshape(slots, tok, local_heads, HEAD_DIM), cosine_table[None], sine[None]
    ).astype(jnp.bfloat16)
    query = query.reshape(slots, tok, local_kv, group, HEAD_DIM)
    scores = jnp.einsum("mtkgd,skd->mkgts", query, keys, preferred_element_type=jnp.float32) * scale
    causal = jnp.arange(tok)[:, None] >= jnp.arange(tok)[None, :]
    scores = jnp.where(causal, scores, -1e30)
    probs = jax.nn.softmax(scores, axis=-1).astype(jnp.bfloat16)
    mixed = (
        jnp.einsum("mkgts,skd->mtkgd", probs, values, preferred_element_type=jnp.float32)
        .astype(jnp.bfloat16)
        .reshape(slots, tok, local_feats)
    )
    low_out = jnp.einsum("mtf,mfr->mtr", mixed, o_left, preferred_element_type=jnp.float32)
    right_full = o_right.astype(jnp.float32)
    part = jnp.einsum(
        "mtf,fe->mte",
        mixed,
        lax.all_gather(w_out, "pop", axis=1, tiled=True),
        preferred_element_type=jnp.float32,
    )
    term = part + factor * jnp.einsum(
        "mtr,mre->mte", low_out, right_full, precision=lax.Precision.HIGHEST
    )
    output = lax.psum_scatter(
        term.astype(jnp.bfloat16), "mp", scatter_dimension=2, tiled=True
    ).astype(jnp.float32)
    diff = output - target.astype(jnp.float32)[None]
    errors = lax.psum(jnp.sum(diff * diff, axis=(1, 2)), "mp")
    fitness = -(errors / (tok * tokens.shape[1]))
    count = slots * lax.axis_size("pop")
    mean = lax.psum(jnp.sum(fitness), "pop") / count
    spread = lax.psum(jnp.sum((fitness - mean) * (fitness - mean)), "pop") / count
    weight = signs * (fitness - mean) / jnp.sqrt(spread + spread_floor)
    every_weight = lax.all_gather(weight, "pop", axis=0, tiled=True)
    right_factors_gathered, left_all = (
        lax.all_gather(query_right_factors, "pop", axis=0, tiled=True),
        lax.all_gather(o_left, "pop", axis=0, tiled=True),
    )
    rows_q = lax.all_to_all(query_left_factors, "pop", split_axis=1, concat_axis=0, tiled=True)
    cols_o = lax.all_to_all(o_right, "pop", split_axis=2, concat_axis=0, tiled=True)
    whole_population = rows_q.shape[0]
    left_q = jnp.transpose(
        rows_q.astype(jnp.float32) * every_weight[:, None, None], (1, 0, 2)
    ).reshape(rows_q.shape[1], whole_population * RANK)
    right_q = right_factors_gathered.astype(jnp.float32).reshape(
        whole_population * RANK, local_feats
    )
    grad_query = jnp.dot(left_q, right_q, precision=lax.Precision.HIGHEST) / noise_scale
    output_left_factor = jnp.transpose(
        left_all.astype(jnp.float32) * every_weight[:, None, None], (1, 0, 2)
    ).reshape(local_feats, whole_population * RANK)
    right_o = cols_o.astype(jnp.float32).reshape(whole_population * RANK, cols_o.shape[2])
    grad_out = jnp.dot(output_left_factor, right_o, precision=lax.Precision.HIGHEST) / noise_scale
    return (grad_query, grad_out, fitness)


def group_of(w_query, w_key):
    return w_query.shape[1] // w_key.shape[1]


def pick(args, n_pop, n_mp):
    tok = args[0].shape[0]
    kernel = (
        args[6].shape[0] == n_pop
        and n_pop % n_mp == 0
        and n_pop % 2 == 0
        and n_pop * PACK <= 128
        and tok % (n_pop * 16) == 0
        and tok // n_pop < 128
        and args[2].shape[1] // n_mp == 2 * args[5].shape[1] // n_pop
        and args[2].shape[0] == args[5].shape[1]
        and args[3].shape[1] == n_mp * HEAD_DIM
    )
    return functools.partial(per_device_fast, n_pop, n_mp) if kernel else per_device


def solution(mesh):
    placed = (
        P(),
        P(None, "mp"),
        P("pop", "mp"),
        P(None, "mp"),
        P(None, "mp"),
        P("mp", "pop"),
        P("pop", None, None),
        P("pop", None, "mp"),
        P("pop", "mp", None),
        P("pop", None, None),
        P("pop"),
    )
    n_pop, n_mp = mesh.shape["pop"], mesh.shape["mp"]

    def whole(*args):
        return jax.shard_map(
            pick(args, n_pop, n_mp),
            mesh=mesh,
            in_specs=placed,
            out_specs=(P("pop", "mp"), P("mp", "pop"), P("pop")),
            check_vma=False,
        )(*args)

    return whole
```
